32 devices in a mesh: scan: 2 (over y), ang: 4 (over z), row: 4 (over x, core).
Axes of the slice: x: 2, y: 2, z: 4, core: 2. Of those that a mesh axis runs over, the one named last changes fastest.
Arguments:
- projections: bfloat16 [8, 32, 2560], P(('scan', 'ang'), 'row'), parts along dimension 0, may hold values from 0 to 2
- flats: float32 [64, 2560], P(('scan', 'row')), parts along dimension 0, may hold values from 1 to 3
- block_start: int32 [4, 4], replicated, may hold values from 0 to 2528
- bp_weights: bfloat16 [4, 32, 1024], P(None, None, 'ang'), may hold values from -0.5 to 0.5
Outputs:
- recon: float32 [64, 1024], P(('scan', 'row'), 'ang'), parts along dimension 0
The draws below stay inside these ranges and needn't reach their ends.
There are 2 independent parts, one for each index of `scan`. The reference program is written for one: setup_inputs(seed, part) draws one part's arguments, and reference() takes and returns one part's arrays. A program takes and returns all parts, laid end to end along the dimension named above; an argument that names none is the same for every part. Nothing has to cross between parts.
Inputs may be any that keep to these rules, and one draw needn't show every extreme that they name: block_start[a, r] is the first of the 32 detector columns that pixel region r reads at angle a.
All inputs are finite; a program needn't handle non-finite values.
Results may differ from the reference program's by a relative error of at most 0.009.
Values may be sent and summed in bfloat16 or wider, within the bound.
A program may use at most 64 MiB of HBM per device.

```python
import math
import jax
import jax.numpy as jnp
from jax import lax

W = 2560
RD = 8
HALO = 4
CB = 32
PIX_DEV = 256
TILE = 16
ANGLES = 4
SLICES = 32
REGIONS = 4
PIX = 1024


def set_ends(entries, stream_key, smallest, largest):
    shape = entries.shape
    spot = [jax.random.randint(jax.random.fold_in(stream_key, axis), (), 0, shape[axis]) for axis in range(len(shape))]
    entries = entries.at[tuple(spot)].set(smallest)
    longest = shape.index(max(shape))
    spot[longest] = (spot[longest] + 1) % shape[longest]
    return entries.at[tuple(spot)].set(largest)


def levels(rng, extent, shards, least, largest):
    factor_of = 1.0
    for position, shards_of in shards:
        steps = jax.random.uniform(jax.random.fold_in(jax.random.fold_in(rng, 6), position), (shards_of,), jnp.float32, least / len(shards), largest / len(shards))
        factor_of = factor_of * jnp.repeat(jnp.exp(steps), extent[position] // shards_of).reshape((-1,) + (1,) * (len(extent) - 1 - position))
    return factor_of


def gaussian(own_key, dims, scale, bound, shards=(), kind=jnp.bfloat16):
    array = jax.random.normal(own_key, dims, jnp.float32) * scale
    if len(shards) > 0:
        array = levels(own_key, dims, shards, -0.22, 0.18) * array
    return jnp.clip(array, min=-bound, max=bound).astype(kind)


def setup_inputs(seed: int = 0, part: int = 0) -> dict:
    keys = jax.random.split(jax.random.key(seed), 5)
    part_splits = jax.random.split(jax.random.fold_in(keys[4], part), 5)
    projections = jnp.clip(2.0 * jax.random.uniform(part_splits[0], (ANGLES, SLICES, W), jnp.float32) ** levels(part_splits[0], (ANGLES, SLICES, W), ((0, 4), (1, 4)), -0.2, 0.2), 0.0, 2.0).astype(jnp.bfloat16)
    flats = jnp.clip(jnp.exp(math.log(3.0) - 1.0986123 * jax.random.uniform(part_splits[1], (SLICES, W), jnp.float32) ** levels(part_splits[1], (SLICES, W), ((0, 4),), -0.2, 0.2)), 1.0, 3.0)
    block_start = set_ends(jax.random.randint(keys[2], (ANGLES, REGIONS), 0, W - CB + 1), jax.random.fold_in(keys[2], 1), 0, W - CB).astype(jnp.int32)
    bp_weights = gaussian(keys[3], (ANGLES, CB, PIX), (ANGLES * CB) ** -0.5, 0.5, ((2, 4),))
    return dict(projections=projections, flats=flats, block_start=block_start, bp_weights=bp_weights)


paganin_beta = 8.0
ramp_gain = 320.0


def reference(projections, flats, block_start, bp_weights):
    contrast = 1.0 - projections.astype(jnp.float32) / flats[None, :, :]
    padded = jnp.pad(contrast, ((0, 0), (HALO, HALO), (0, 0)))
    tile_count = SLICES // RD
    row_index = (jnp.arange(tile_count, dtype=jnp.int32)[:, None] * RD
                 + jnp.arange(TILE, dtype=jnp.int32)[None, :]).astype(jnp.int32)
    row_freq = jnp.arange(TILE, dtype=jnp.float32)
    col_freq = jnp.arange(W, dtype=jnp.float32)
    lam = (4.0 * jnp.sin(jnp.pi * row_freq / TILE) ** 2)[:, None] + (4.0 * jnp.sin(jnp.pi * col_freq / W) ** 2)[None, :]
    filt = 1.0 / (1.0 + paganin_beta * lam)
    folded = jnp.minimum(col_freq, W - col_freq)
    ramp = ramp_gain * (folded / W) * (0.5 + 0.5 * jnp.cos(2.0 * jnp.pi * folded / W))

    def one_angle(angle_rows):
        tiles = angle_rows[row_index]
        spectrum = jnp.fft.fft2(tiles, axes=(1, 2)) * filt
        back = jnp.real(jnp.fft.ifft2(spectrum, axes=(1, 2)))
        paganin = back[:, HALO:HALO + RD, :].reshape(SLICES, W)
        filtered = jnp.real(jnp.fft.ifft(jnp.fft.fft(paganin, axis=-1) * ramp, axis=-1))
        return filtered.astype(jnp.bfloat16)

    sinogram = lax.map(one_angle, padded)
    offsets = jnp.arange(CB, dtype=jnp.int32)

    def one_region(region):
        starts = lax.dynamic_index_in_dim(block_start, region, 1, keepdims=False)
        index = (starts[:, None] + offsets[None, :]).astype(jnp.int32)
        index = jnp.broadcast_to(index[:, None, :], (ANGLES, SLICES, CB))
        blocks = jnp.take_along_axis(sinogram, index, axis=2)
        weights = lax.dynamic_slice_in_dim(bp_weights, region * PIX_DEV, PIX_DEV, 2)
        return jnp.einsum('asc,acp->sp', blocks.astype(jnp.float32), weights.astype(jnp.float32))

    parts = lax.map(one_region, jnp.arange(REGIONS, dtype=jnp.int32))
    return jnp.transpose(parts, (1, 0, 2)).reshape(SLICES, PIX)
```

```python
import functools

import jax
import jax.numpy as jnp
import numpy as np
from jax import lax
from jax.experimental import pallas as pl
from jax.experimental.pallas import tpu as pltpu
from jax.sharding import PartitionSpec as P

HALO = 4
LANES = 128
paganin_beta = 8.0
ramp_gain = 320.0


def filter_table(tile_rows, width, columns):
    u = np.arange(tile_rows, dtype=np.float64)
    v = np.arange(width, dtype=np.float64)
    lam = (4.0 * np.sin(np.pi * u / tile_rows) ** 2)[:, None] + (4.0 * np.sin(np.pi * v / width) ** 2)[None, :]
    folded = np.minimum(v, width - v)
    ramp = ramp_gain * (folded / width) * (0.5 + 0.5 * np.cos(2.0 * np.pi * folded / width))
    taps = np.real(np.fft.ifft2(ramp[None, :] / (1.0 + paganin_beta * lam)))
    lags = tile_rows // 2 + 1
    place = (np.arange(columns)[:, None] - np.arange(width)[None, :]) % width
    return taps[:lags][:, place].reshape(lags * columns, width)


def kernel(regions, tiles, starts, proj, flats, table, weights, out,
           starts_s, proj_v, flats_v, table_v, weights_v, xs, ys, sbuf, rbuf,
           load_sem, send_sem, recv_sem):
    rows, width = flats.shape
    blocks = width // LANES
    angles, cb, _ = weights.shape
    half = rows // 2
    cs = LANES // rows
    shifts = cb // cs
    me = lax.axis_index("ang")
    row = lax.axis_index("row")

    def peer(step, delta):
        return {"ang": lax.rem(me + step, regions), "row": lax.rem(row + delta + tiles, tiles)}

    links = [(step, delta) for step in (*range(1, regions), 0) for delta in (-1, 1, 0) if (step, delta) != (0, 0)]

    def when_there(delta, action):
        if delta == 0:
            action()
        else:
            pl.when(row > 0 if delta < 0 else row < tiles - 1)(action)

    loads = [pltpu.make_async_copy(proj.at[0], proj_v, load_sem.at[0]),
             pltpu.make_async_copy(flats, flats_v, load_sem.at[1]),
             pltpu.make_async_copy(starts, starts_s, load_sem.at[3])]
    table_load = pltpu.make_async_copy(table, table_v, load_sem.at[4])
    weight_load = pltpu.make_async_copy(weights, weights_v, load_sem.at[2])
    for copy in [*loads, table_load, weight_load]:
        copy.start()

    barrier = pltpu.get_barrier_semaphore()
    for step, delta in links:
        when_there(delta, lambda: pl.semaphore_signal(
            barrier, inc=1, device_id=peer(step, delta), device_id_type=pl.DeviceIdType.MESH))

    def slot(delta):
        return pl.ds((1 + delta) * rows, rows)

    zeros = jnp.zeros((angles, rows, shifts * LANES), jnp.bfloat16)
    pl.when(row == tiles - 1)(lambda: rbuf.at[:, slot(-1)].__setitem__(..., zeros))
    pl.when(row == 0)(lambda: rbuf.at[:, slot(1)].__setitem__(..., zeros))

    lane = lax.broadcasted_iota(jnp.int32, (rows, LANES), 1)
    sub = lax.broadcasted_iota(jnp.int32, (rows, LANES), 0)

    for copy in loads:
        copy.wait()

    pieces = [slice(b * LANES, (b + 1) * LANES) for b in range(blocks)]
    contrast = [1.0 - proj_v[:, p].astype(jnp.float32) / flats_v[:, p] for p in pieces]
    mean = jnp.sum(sum(contrast), axis=1, keepdims=True) / width
    for b, x in enumerate(contrast):
        xs[b] = x - mean
        xs[b + blocks] = x - mean

    for g in range(regions):
        shifted = []
        for k in range(shifts):
            start = starts_s[me, g] + k * cs
            first = start // LANES
            rest = lax.rem(start, LANES)
            shift = lax.rem(LANES - rest, LANES)
            low = lane < LANES - rest
            turned = [pltpu.roll(xs[first + b], shift, 1) for b in range(blocks + 1)]
            shifted.append([jnp.where(low, turned[b], turned[b + 1]) for b in range(blocks)])
        for b in range(blocks):
            ys[g * shifts * rows:(g + 1) * shifts * rows, b * LANES:(b + 1) * LANES] = jnp.concatenate(
                [y[b] for y in shifted], axis=0).astype(jnp.bfloat16)

    table_load.wait()
    total = lax.dot_general(ys[...], table_v[...], (((1,), (1,)), ((), ())), preferred_element_type=jnp.float32)
    total = jnp.concatenate([total, jnp.zeros((total.shape[0], LANES - cs), jnp.float32)], axis=1)

    lag = lane // cs
    up, down = lax.rem(sub + rows - lag, rows), lax.rem(sub + lag, rows)
    inside = [sub >= lag, (lag > 0) & (sub + lag < rows)]
    wrapped = [(sub < lag) | (lag == 0), sub + lag >= rows]
    parts = {0: inside,
             -1: [wrapped[0] & (up < half), wrapped[1] & (down < half)],
             1: [wrapped[0] & (up >= half), wrapped[1] & (down >= half)]}
    bits = [1 << n for n in range((rows - 1).bit_length())]
    for g in range(regions):
        for k in range(shifts):
            base = (g * shifts + k) * rows
            tile = total[base:base + rows, :LANES]
            last = total[base:base + rows, LANES:]
            ahead, back = tile, tile
            for bit in bits:
                turn = (lag & bit) > 0
                ahead = jnp.where(turn, pltpu.roll(ahead, bit, 0), ahead)
                back = jnp.where(turn, pltpu.roll(back, rows - bit, 0), back)
            edge = jnp.where(lag == 0, last, ahead)
            for delta, (first, second) in parts.items():
                value = jnp.where(first, edge if delta else ahead, 0.0) + jnp.where(second, back, 0.0)
                sbuf[1 + delta, g, :, k * LANES:(k + 1) * LANES] = value.astype(jnp.bfloat16)

    sides = (row > 0).astype(jnp.int32) + (row < tiles - 1).astype(jnp.int32)
    pl.semaphore_wait(barrier, regions - 1 + sides * regions)

    for step, delta in links:
        to = peer(step, delta)
        copy = pltpu.make_async_remote_copy(
            src_ref=sbuf.at[1 + delta, to["ang"]], dst_ref=rbuf.at[me, slot(delta)],
            send_sem=send_sem.at[1 + delta], recv_sem=recv_sem.at[1 + delta],
            device_id=to, device_id_type=pl.DeviceIdType.MESH)
        when_there(delta, copy.start)
    weight_load.wait()
    rbuf[me, slot(0)] = sbuf[1, me]

    def group(delta):
        count = angles - 1 if delta == 0 else angles
        return pltpu.make_async_remote_copy(
            src_ref=sbuf.at[1 + delta, pl.ds(0, count)], dst_ref=rbuf.at[pl.ds(0, count), slot(delta)],
            send_sem=send_sem.at[1 + delta], recv_sem=recv_sem.at[1 + delta],
            device_id=peer(1, delta), device_id_type=pl.DeviceIdType.MESH)

    for delta in (0, -1, 1):
        when_there(-delta, group(delta).wait_recv)

    result = jnp.zeros((3 * rows, out.shape[1]), jnp.float32)
    for a in range(angles):
        w = jnp.concatenate([weights_v[a, k * cs:(k + 1) * cs] for k in range(shifts) for _ in range(rows)], axis=0)
        result = result + jnp.dot(rbuf[a], w, preferred_element_type=jnp.float32)
    out[...] = result[:rows] + result[rows:2 * rows] + result[2 * rows:]
    for delta in (0, -1, 1):
        when_there(delta, group(delta).wait_send)


def body(projections, flats, block_start, bp_weights):
    _, rows, width = projections.shape
    angles, cb, pixels = bp_weights.shape
    regions, tiles = lax.axis_size("ang"), lax.axis_size("row")
    cs = LANES // rows
    shifts = cb // cs
    table = jnp.asarray(filter_table(rows + 2 * HALO, width, cs), jnp.bfloat16)
    hbm = pl.BlockSpec(memory_space=pltpu.HBM)
    return pl.pallas_call(
        functools.partial(kernel, regions, tiles),
        name="fbp",
        out_shape=pltpu.VMEM((rows, pixels), jnp.float32),
        in_specs=[hbm, hbm, hbm, hbm, hbm],
        out_specs=pl.BlockSpec(memory_space=pltpu.VMEM),
        scratch_shapes=[
            pltpu.SMEM(block_start.shape, jnp.int32),
            pltpu.VMEM((rows, width), jnp.bfloat16),
            pltpu.VMEM((rows, width), jnp.float32),
            pltpu.VMEM(table.shape, jnp.bfloat16),
            pltpu.VMEM(bp_weights.shape, jnp.bfloat16),
            pltpu.VMEM((2 * width // LANES, rows, LANES), jnp.float32),
            pltpu.VMEM((regions * shifts * rows, width), jnp.bfloat16),
            pltpu.VMEM((3, regions, rows, shifts * LANES), jnp.bfloat16),
            pltpu.VMEM((angles, 3 * rows, shifts * LANES), jnp.bfloat16),
            pltpu.SemaphoreType.DMA((5,)),
            pltpu.SemaphoreType.DMA((3,)),
            pltpu.SemaphoreType.DMA((3,)),
        ],
        compiler_params=pltpu.CompilerParams(collective_id=0, has_side_effects=True, vmem_limit_bytes=65000000),
    )(block_start, projections, flats, table, bp_weights)


def solution(mesh):
    placed = (P(("scan", "ang"), "row", None), P(("scan", "row"), None), P(), P(None, None, "ang"))
    return jax.shard_map(
        body, mesh=mesh, in_specs=placed, out_specs=P(("scan", "row"), "ang"), check_vma=False
    )
```

```python
import functools

import jax
import jax.numpy as jnp
import numpy as np
from jax import lax
from jax.experimental import pallas as pl
from jax.experimental.pallas import tpu as pltpu
from jax.sharding import PartitionSpec as P

HALO = 4
LANES = 128
FLAT_CUTS = 4
PROJ_CUTS = 2
CENTRE = 4
paganin_beta = 8.0
ramp_gain = 320.0


def filter_table(tile_rows, width, columns):
    u = np.arange(tile_rows, dtype=np.float64)
    v = np.arange(width, dtype=np.float64)
    lam = (4.0 * np.sin(np.pi * u / tile_rows) ** 2)[:, None] + (4.0 * np.sin(np.pi * v / width) ** 2)[None, :]
    folded = np.minimum(v, width - v)
    ramp = ramp_gain * (folded / width) * (0.5 + 0.5 * np.cos(2.0 * np.pi * folded / width))
    taps = np.real(np.fft.ifft2(ramp[None, :] / (1.0 + paganin_beta * lam)))
    lags = tile_rows // 2 + 1
    place = (np.arange(columns)[:, None] - np.arange(width)[None, :]) % width
    sign = np.where(np.arange(width) < width // LANES // 2 * LANES, 1.0, -1.0)
    return taps[:lags][:, place].reshape(lags * columns, width) * sign


def kernel(regions, tiles, starts, proj, flats, table, weights, out,
           starts_s, proj_v, flats_v, table_v, weights_v, xs, ys, sbuf, rbuf,
           load_sem, send_sem, recv_sem):
    rows, width = flats.shape
    blocks = width // LANES
    angles, cb, _ = weights.shape
    half = rows // 2
    cs = LANES // rows
    shifts = cb // cs
    me = lax.axis_index("ang")
    row = lax.axis_index("row")

    def peer(step, delta):
        return {"ang": lax.rem(me + step, regions), "row": lax.rem(row + delta + tiles, tiles)}

    links = [(step, delta) for step in (*range(1, regions), 0) for delta in (-1, 1, 0) if (step, delta) != (0, 0)]

    def when_there(delta, action):
        if delta == 0:
            action()
        else:
            pl.when(row > 0 if delta < 0 else row < tiles - 1)(action)

    loads = [pltpu.make_async_copy(flats, flats_v, load_sem.at[1]),
             pltpu.make_async_copy(proj.at[0], proj_v, load_sem.at[0]),
             pltpu.make_async_copy(starts, starts_s, load_sem.at[3])]
    table_load = pltpu.make_async_copy(table, table_v, load_sem.at[4])
    weight_load = pltpu.make_async_copy(weights, weights_v, load_sem.at[2])
    for n in range(FLAT_CUTS):
        part = pl.ds(n * width // FLAT_CUTS, width // FLAT_CUTS)
        pltpu.make_async_copy(flats.at[:, part], flats_v.at[:, part], load_sem.at[1]).start()
    for n in range(PROJ_CUTS):
        part = pl.ds(n * width // PROJ_CUTS, width // PROJ_CUTS)
        pltpu.make_async_copy(proj.at[0, :, part], proj_v.at[:, part], load_sem.at[0]).start()
    for copy in [loads[2], table_load, weight_load]:
        copy.start()

    barrier = pltpu.get_barrier_semaphore()
    for step, delta in links:
        when_there(delta, lambda: pl.semaphore_signal(
            barrier, inc=1, device_id=peer(step, delta), device_id_type=pl.DeviceIdType.MESH))

    def slot(delta):
        return pl.ds((1 + delta) * rows, rows)

    zeros = jnp.zeros((angles, rows, shifts * LANES), jnp.bfloat16)
    pl.when(row == tiles - 1)(lambda: rbuf.at[:, slot(-1)].__setitem__(..., zeros))
    pl.when(row == 0)(lambda: rbuf.at[:, slot(1)].__setitem__(..., zeros))

    lane = lax.broadcasted_iota(jnp.int32, (rows, LANES), 1)
    sub = lax.broadcasted_iota(jnp.int32, (rows, LANES), 0)

    for copy in loads:
        copy.wait()

    pieces = [slice(b * LANES, (b + 1) * LANES) for b in range(blocks)]
    contrast = [1.0 - proj_v[:, p].astype(jnp.float32) / flats_v[:, p] for p in pieces]
    centre = jnp.sum(sum(contrast[:CENTRE]), axis=1, keepdims=True) / (CENTRE * LANES)
    for b, x in enumerate(contrast):
        xs[b] = x - centre
        xs[b + blocks] = x - centre

    for g in range(regions):
        shifted = []
        for k in range(shifts):
            start = starts_s[me, g] + k * cs
            first = start // LANES
            rest = lax.rem(start, LANES)
            shift = lax.rem(LANES - rest, LANES)
            low = lane < LANES - rest
            turned = [pltpu.roll(xs[first + b], shift, 1) for b in range(blocks + 1)]
            shifted.append([jnp.where(low, turned[b], turned[b + 1]) for b in range(blocks)])
        for b in range(blocks):
            ys[g * shifts * rows:(g + 1) * shifts * rows, b * LANES:(b + 1) * LANES] = jnp.concatenate(
                [y[b] for y in shifted], axis=0).astype(jnp.bfloat16)

    table_load.wait()
    cut = blocks // 2 * LANES
    near, far = (lax.dot_general(ys[:, part], table_v[:, part], (((1,), (1,)), ((), ())), preferred_element_type=jnp.float32)
                 for part in (slice(cut), slice(cut, width)))
    total = near - far
    total = jnp.concatenate([total, jnp.zeros((total.shape[0], LANES - cs), jnp.float32)], axis=1)

    lag = lane // cs
    up, down = lax.rem(sub + rows - lag, rows), lax.rem(sub + lag, rows)
    inside = [sub >= lag, (lag > 0) & (sub + lag < rows)]
    wrapped = [(sub < lag) | (lag == 0), sub + lag >= rows]
    parts = {0: inside,
             -1: [wrapped[0] & (up < half), wrapped[1] & (down < half)],
             1: [wrapped[0] & (up >= half), wrapped[1] & (down >= half)]}
    bits = [1 << n for n in range((rows - 1).bit_length())]
    for g in range(regions):
        for k in range(shifts):
            base = (g * shifts + k) * rows
            tile = total[base:base + rows, :LANES]
            last = total[base:base + rows, LANES:]
            ahead, back = tile, tile
            for bit in bits:
                turn = (lag & bit) > 0
                ahead = jnp.where(turn, pltpu.roll(ahead, bit, 0), ahead)
                back = jnp.where(turn, pltpu.roll(back, rows - bit, 0), back)
            edge = jnp.where(lag == 0, last, ahead)
            for delta, (first, second) in parts.items():
                value = jnp.where(first, edge if delta else ahead, 0.0) + jnp.where(second, back, 0.0)
                sbuf[1 + delta, g, :, k * LANES:(k + 1) * LANES] = value.astype(jnp.bfloat16)

    sides = (row > 0).astype(jnp.int32) + (row < tiles - 1).astype(jnp.int32)
    pl.semaphore_wait(barrier, regions - 1 + sides * regions)

    for step, delta in links:
        to = peer(step, delta)
        copy = pltpu.make_async_remote_copy(
            src_ref=sbuf.at[1 + delta, to["ang"]], dst_ref=rbuf.at[me, slot(delta)],
            send_sem=send_sem.at[1 + delta], recv_sem=recv_sem.at[me],
            device_id=to, device_id_type=pl.DeviceIdType.MESH)
        when_there(delta, copy.start)
    weight_load.wait()
    rbuf[me, slot(0)] = sbuf[1, me]

    def sent(delta):
        count = regions - 1 if delta == 0 else regions
        return pltpu.make_async_remote_copy(
            src_ref=sbuf.at[1 + delta, pl.ds(0, count)], dst_ref=rbuf.at[pl.ds(0, count), slot(delta)],
            send_sem=send_sem.at[1 + delta], recv_sem=recv_sem.at[me],
            device_id=peer(1, delta), device_id_type=pl.DeviceIdType.MESH)

    inner = (row > 0) & (row < tiles - 1)
    turn = jnp.where(me < regions // 2, 1, regions - 1)

    def source(step):
        return lax.rem(me + step * turn, regions)

    def arrived(step):
        angle = source(step)

        def wait(count):
            pltpu.make_async_remote_copy(
                src_ref=rbuf.at[angle, pl.ds(0, count * rows)], dst_ref=rbuf.at[angle, pl.ds(0, count * rows)],
                send_sem=send_sem.at[0], recv_sem=recv_sem.at[angle],
                device_id=peer(1, 0), device_id_type=pl.DeviceIdType.MESH).wait_recv()

        own = 1 if step == 0 else 0
        pl.when(inner)(lambda: wait(3 - own))
        pl.when(jnp.logical_not(inner))(lambda: wait(2 - own))

    def projected(steps):
        sums = []
        for half_pixels in range(2):
            pixels = pl.ds(half_pixels * (out.shape[1] // 2), out.shape[1] // 2)
            result = 0.0
            for step in steps:
                angle = source(step)
                w = jnp.concatenate(
                    [weights_v[angle, k * cs:(k + 1) * cs, pixels] for k in range(shifts) for _ in range(rows)], axis=0)
                result += jnp.dot(rbuf[angle], w, preferred_element_type=jnp.float32)
            sums.append(result[:rows] + result[rows:2 * rows] + result[2 * rows:])
        return jnp.concatenate(sums, axis=1)

    for step in range(regions - 1):
        arrived(step)
    out[...] = projected(range(regions - 1))
    arrived(regions - 1)
    out[...] += projected([regions - 1])
    for delta in (0, -1, 1):
        when_there(delta, sent(delta).wait_send)


def body(projections, flats, block_start, bp_weights):
    _, rows, width = projections.shape
    angles, cb, pixels = bp_weights.shape
    regions, tiles = lax.axis_size("ang"), lax.axis_size("row")
    cs = LANES // rows
    shifts = cb // cs
    table = jnp.asarray(filter_table(rows + 2 * HALO, width, cs), jnp.bfloat16)
    hbm = pl.BlockSpec(memory_space=pltpu.HBM)
    return pl.pallas_call(
        functools.partial(kernel, regions, tiles),
        name="fbp",
        out_shape=pltpu.VMEM((rows, pixels), jnp.float32),
        in_specs=[hbm, hbm, hbm, hbm, hbm],
        out_specs=pl.BlockSpec(memory_space=pltpu.VMEM),
        scratch_shapes=[
            pltpu.SMEM(block_start.shape, jnp.int32),
            pltpu.VMEM((rows, width), jnp.bfloat16),
            pltpu.VMEM((rows, width), jnp.float32),
            pltpu.VMEM(table.shape, jnp.bfloat16),
            pltpu.VMEM(bp_weights.shape, jnp.bfloat16),
            pltpu.VMEM((2 * width // LANES, rows, LANES), jnp.float32),
            pltpu.VMEM((regions * shifts * rows, width), jnp.bfloat16),
            pltpu.VMEM((3, regions, rows, shifts * LANES), jnp.bfloat16),
            pltpu.VMEM((angles, 3 * rows, shifts * LANES), jnp.bfloat16),
            pltpu.SemaphoreType.DMA((5,)),
            pltpu.SemaphoreType.DMA((3,)),
            pltpu.SemaphoreType.DMA((angles,)),
        ],
        compiler_params=pltpu.CompilerParams(collective_id=0, has_side_effects=True, vmem_limit_bytes=65000000),
    )(block_start, projections, flats, table, bp_weights)


def solution(mesh):
    placed = (P(("scan", "ang"), "row", None), P(("scan", "row"), None), P(), P(None, None, "ang"))
    return jax.shard_map(
        body, mesh=mesh, in_specs=placed, out_specs=P(("scan", "row"), "ang"), check_vma=False
    )
```

```python
import functools

import jax
import jax.numpy as jnp
import numpy as np
from jax import lax
from jax.experimental import pallas as pl
from jax.experimental.pallas import tpu as pltpu
from jax.sharding import PartitionSpec as P

HALO = 4
LANES = 128
FLAT_CUTS = 4
PROJ_CUTS = 2
CENTRE = 4
paganin_beta = 8.0
ramp_gain = 320.0


def filter_table(tile_rows, width, columns):
    u = np.arange(tile_rows, dtype=np.float64)
    v = np.arange(width, dtype=np.float64)
    lam = (4.0 * np.sin(np.pi * u / tile_rows) ** 2)[:, None] + (4.0 * np.sin(np.pi * v / width) ** 2)[None, :]
    folded = np.minimum(v, width - v)
    ramp = ramp_gain * (folded / width) * (0.5 + 0.5 * np.cos(2.0 * np.pi * folded / width))
    taps = np.real(np.fft.ifft2(ramp[None, :] / (1.0 + paganin_beta * lam)))
    lags = tile_rows // 2 + 1
    place = (np.arange(columns)[:, None] - np.arange(width)[None, :]) % width
    sign = np.where(np.arange(width) < width // LANES // 2 * LANES, 1.0, -1.0)
    return taps[:lags][:, place].reshape(lags * columns, width) * sign


def kernel(regions, tiles, starts, proj, flats, table, weights, out,
           starts_s, proj_v, flats_v, table_v, weights_v, xs, ys, sbuf, rbuf,
           load_sem, send_sem, recv_sem):
    rows, width = flats.shape
    blocks = width // LANES
    angles, cb, _ = weights.shape
    half = rows // 2
    cs = LANES // rows
    shifts = cb // cs
    me = lax.axis_index("ang")
    row = lax.axis_index("row")

    def peer(step, delta):
        return {"ang": lax.rem(me + step, regions), "row": lax.rem(row + delta + tiles, tiles)}

    links = [(step, delta) for step in (*range(1, regions), 0) for delta in (-1, 1, 0) if (step, delta) != (0, 0)]

    def when_there(delta, action):
        if delta == 0:
            action()
        else:
            pl.when(row > 0 if delta < 0 else row < tiles - 1)(action)

    loads = [pltpu.make_async_copy(flats, flats_v, load_sem.at[1]),
             pltpu.make_async_copy(proj.at[0], proj_v, load_sem.at[0]),
             pltpu.make_async_copy(starts, starts_s, load_sem.at[3])]
    lags = rows + 1
    table_load = pltpu.make_async_copy(table, table_v.at[pl.ds(0, lags * rows)], load_sem.at[4])
    weight_load = pltpu.make_async_copy(weights, weights_v, load_sem.at[2])
    for n in range(FLAT_CUTS):
        part = pl.ds(n * width // FLAT_CUTS, width // FLAT_CUTS)
        pltpu.make_async_copy(flats.at[:, part], flats_v.at[:, part], load_sem.at[1]).start()
    for n in range(PROJ_CUTS):
        part = pl.ds(n * width // PROJ_CUTS, width // PROJ_CUTS)
        pltpu.make_async_copy(proj.at[0, :, part], proj_v.at[:, part], load_sem.at[0]).start()
    loads[2].start()
    for d in range(lags):
        pltpu.make_async_copy(table.at[pl.ds(d * rows, rows)], table_v.at[pl.ds(d * cs, rows)], load_sem.at[4]).start()
    weight_load.start()

    barrier = pltpu.get_barrier_semaphore()
    for step, delta in links:
        when_there(delta, lambda: pl.semaphore_signal(
            barrier, inc=1, device_id=peer(step, delta), device_id_type=pl.DeviceIdType.MESH))

    def slot(delta):
        return pl.ds((1 + delta) * rows, rows)

    zeros = jnp.zeros((angles, rows, shifts * LANES), jnp.bfloat16)
    pl.when(row == tiles - 1)(lambda: rbuf.at[:, slot(-1)].__setitem__(..., zeros))
    pl.when(row == 0)(lambda: rbuf.at[:, slot(1)].__setitem__(..., zeros))

    lane = lax.broadcasted_iota(jnp.int32, (rows, LANES), 1)
    sub = lax.broadcasted_iota(jnp.int32, (rows, LANES), 0)

    for copy in loads:
        copy.wait()

    pieces = [slice(b * LANES, (b + 1) * LANES) for b in range(blocks)]
    contrast = [1.0 - proj_v[:, p].astype(jnp.float32) / flats_v[:, p] for p in pieces]
    centre = jnp.sum(sum(contrast[:CENTRE]), axis=1, keepdims=True) / (CENTRE * LANES)
    for b, x in enumerate(contrast):
        xs[b] = x - centre
        xs[b + blocks] = x - centre

    table_load.wait()
    for g in range(regions):
        shifted = []
        for k in range(shifts):
            start = starts_s[me, g] + k * cs
            first = start // LANES
            rest = lax.rem(start, LANES)
            shift = lax.rem(LANES - rest, LANES)
            low = lane < LANES - rest
            turned = [pltpu.roll(xs[first + b], shift, 1) for b in range(blocks + 1)]
            shifted.append([jnp.where(low, turned[b], turned[b + 1]) for b in range(blocks)])
        for b in range(blocks):
            ys[g * shifts * rows:(g + 1) * shifts * rows, b * LANES:(b + 1) * LANES] = jnp.concatenate(
                [y[b] for y in shifted], axis=0).astype(jnp.bfloat16)

    cut = blocks // 2
    wide = lax.broadcasted_iota(jnp.int32, (2 * rows, LANES), 1)
    for d in range(0, lags, 2):
        pair = [e for e in (d, d + 1) if e < lags]
        turned = [pltpu.roll(jnp.concatenate([table_v[e * cs:e * cs + rows, p] for e in pair], axis=0).astype(jnp.float32), rows, 1)
                  for p in pieces]
        for b, p in enumerate(pieces):
            before = -turned[b - 1] if b in (0, cut) else turned[b - 1]
            value = jnp.where(wide[:len(pair) * rows] < rows, before, turned[b]).astype(jnp.bfloat16)
            for n, e in enumerate(pair):
                table_v[e * cs + rows:(e + 1) * cs, p] = value[n * rows:(n + 1) * rows]
    cut = cut * LANES
    near, far = (lax.dot_general(ys[:, part], table_v[:, part], (((1,), (1,)), ((), ())), preferred_element_type=jnp.float32)
                 for part in (slice(cut), slice(cut, width)))
    total = near - far
    total = jnp.concatenate([total, jnp.zeros((total.shape[0], LANES - cs), jnp.float32)], axis=1)

    lag = lane // cs
    up, down = lax.rem(sub + rows - lag, rows), lax.rem(sub + lag, rows)
    inside = [sub >= lag, (lag > 0) & (sub + lag < rows)]
    wrapped = [(sub < lag) | (lag == 0), sub + lag >= rows]
    parts = {0: inside,
             -1: [wrapped[0] & (up < half), wrapped[1] & (down < half)],
             1: [wrapped[0] & (up >= half), wrapped[1] & (down >= half)]}
    bits = [1 << n for n in range((rows - 1).bit_length())]
    for g in range(regions):
        for k in range(shifts):
            base = (g * shifts + k) * rows
            tile = total[base:base + rows, :LANES]
            last = total[base:base + rows, LANES:]
            ahead, back = tile, tile
            for bit in bits:
                turn = (lag & bit) > 0
                ahead = jnp.where(turn, pltpu.roll(ahead, bit, 0), ahead)
                back = jnp.where(turn, pltpu.roll(back, rows - bit, 0), back)
            edge = jnp.where(lag == 0, last, ahead)
            for delta, (first, second) in parts.items():
                value = jnp.where(first, edge if delta else ahead, 0.0) + jnp.where(second, back, 0.0)
                sbuf[1 + delta, g, :, k * LANES:(k + 1) * LANES] = value.astype(jnp.bfloat16)

    sides = (row > 0).astype(jnp.int32) + (row < tiles - 1).astype(jnp.int32)
    pl.semaphore_wait(barrier, regions - 1 + sides * regions)

    for step, delta in links:
        to = peer(step, delta)
        copy = pltpu.make_async_remote_copy(
            src_ref=sbuf.at[1 + delta, to["ang"]], dst_ref=rbuf.at[me, slot(delta)],
            send_sem=send_sem.at[1 + delta], recv_sem=recv_sem.at[me],
            device_id=to, device_id_type=pl.DeviceIdType.MESH)
        when_there(delta, copy.start)
    weight_load.wait()
    rbuf[me, slot(0)] = sbuf[1, me]

    def sent(delta):
        count = regions - 1 if delta == 0 else regions
        return pltpu.make_async_remote_copy(
            src_ref=sbuf.at[1 + delta, pl.ds(0, count)], dst_ref=rbuf.at[pl.ds(0, count), slot(delta)],
            send_sem=send_sem.at[1 + delta], recv_sem=recv_sem.at[me],
            device_id=peer(1, delta), device_id_type=pl.DeviceIdType.MESH)

    inner = (row > 0) & (row < tiles - 1)
    turn = jnp.where(me < regions // 2, 1, regions - 1)

    def source(step):
        return lax.rem(me + step * turn, regions)

    def arrived(step):
        angle = source(step)

        def wait(count):
            pltpu.make_async_remote_copy(
                src_ref=rbuf.at[angle, pl.ds(0, count * rows)], dst_ref=rbuf.at[angle, pl.ds(0, count * rows)],
                send_sem=send_sem.at[0], recv_sem=recv_sem.at[angle],
                device_id=peer(1, 0), device_id_type=pl.DeviceIdType.MESH).wait_recv()

        own = 1 if step == 0 else 0
        pl.when(inner)(lambda: wait(3 - own))
        pl.when(jnp.logical_not(inner))(lambda: wait(2 - own))

    def projected(steps):
        sums = []
        for half_pixels in range(2):
            pixels = pl.ds(half_pixels * (out.shape[1] // 2), out.shape[1] // 2)
            result = 0.0
            for step in steps:
                angle = source(step)
                w = jnp.concatenate(
                    [weights_v[angle, k * cs:(k + 1) * cs, pixels] for k in range(shifts) for _ in range(rows)], axis=0)
                result += jnp.dot(rbuf[angle], w, preferred_element_type=jnp.float32)
            sums.append(result[:rows] + result[rows:2 * rows] + result[2 * rows:])
        return jnp.concatenate(sums, axis=1)

    for step in range(regions - 1):
        arrived(step)
    out[...] = projected(range(regions - 1))
    arrived(regions - 1)
    out[...] += projected([regions - 1])
    for delta in (0, -1, 1):
        when_there(delta, sent(delta).wait_send)


def body(projections, flats, block_start, bp_weights):
    _, rows, width = projections.shape
    angles, cb, pixels = bp_weights.shape
    regions, tiles = lax.axis_size("ang"), lax.axis_size("row")
    cs = LANES // rows
    shifts = cb // cs
    table = jnp.asarray(filter_table(rows + 2 * HALO, width, rows), jnp.bfloat16)
    lags = table.shape[0] // rows
    hbm = pl.BlockSpec(memory_space=pltpu.HBM)
    return pl.pallas_call(
        functools.partial(kernel, regions, tiles),
        name="fbp",
        out_shape=pltpu.VMEM((rows, pixels), jnp.float32),
        in_specs=[hbm, hbm, hbm, hbm, hbm],
        out_specs=pl.BlockSpec(memory_space=pltpu.VMEM),
        scratch_shapes=[
            pltpu.SMEM(block_start.shape, jnp.int32),
            pltpu.VMEM((rows, width), jnp.bfloat16),
            pltpu.VMEM((rows, width), jnp.float32),
            pltpu.VMEM((lags * cs, width), jnp.bfloat16),
            pltpu.VMEM(bp_weights.shape, jnp.bfloat16),
            pltpu.VMEM((2 * width // LANES, rows, LANES), jnp.float32),
            pltpu.VMEM((regions * shifts * rows, width), jnp.bfloat16),
            pltpu.VMEM((3, regions, rows, shifts * LANES), jnp.bfloat16),
            pltpu.VMEM((angles, 3 * rows, shifts * LANES), jnp.bfloat16),
            pltpu.SemaphoreType.DMA((5,)),
            pltpu.SemaphoreType.DMA((3,)),
            pltpu.SemaphoreType.DMA((angles,)),
        ],
        compiler_params=pltpu.CompilerParams(collective_id=0, has_side_effects=True, vmem_limit_bytes=65000000),
    )(block_start, projections, flats, table, bp_weights)


def solution(mesh):
    placed = (P(("scan", "ang"), "row", None), P(("scan", "row"), None), P(), P(None, None, "ang"))
    return jax.shard_map(
        body, mesh=mesh, in_specs=placed, out_specs=P(("scan", "row"), "ang"), check_vma=False
    )
```

```python
import functools

import jax
import jax.numpy as jnp
import numpy as np
from jax import lax
from jax.experimental import pallas as pl
from jax.experimental.pallas import tpu as pltpu
from jax.sharding import PartitionSpec as P

HALO = 4
LANES = 128
FLAT_CUTS = 2
TABLE_CUTS = 2
CENTRE = 4
paganin_beta = 8.0
ramp_gain = 320.0


def filter_table(tile_rows, width, columns):
    u = np.arange(tile_rows, dtype=np.float64)
    v = np.arange(width, dtype=np.float64)
    lam = (4.0 * np.sin(np.pi * u / tile_rows) ** 2)[:, None] + (4.0 * np.sin(np.pi * v / width) ** 2)[None, :]
    folded = np.minimum(v, width - v)
    ramp = ramp_gain * (folded / width) * (0.5 + 0.5 * np.cos(2.0 * np.pi * folded / width))
    taps = np.real(np.fft.ifft2(ramp[None, :] / (1.0 + paganin_beta * lam)))
    lags = tile_rows // 2 + 1
    place = (np.arange(columns)[:, None] - np.arange(width)[None, :]) % width
    sign = np.where(np.arange(width) < width // LANES // 2 * LANES, 1.0, -1.0)
    return taps[:lags][:, place].reshape(lags * columns, width) * sign


def kernel(regions, tiles, starts, proj, flats, table, weights, out,
           starts_s, proj_v, flats_v, table_v, weights_v, xs, ys, sbuf, rbuf,
           load_sem, send_sem, recv_sem):
    rows, width = flats.shape
    blocks = width // LANES
    angles, cb, _ = weights.shape
    half = rows // 2
    cs = LANES // rows
    shifts = cb // cs
    me = lax.axis_index("ang")
    row = lax.axis_index("row")

    def peer(step, delta):
        return {"ang": lax.rem(me + step, regions), "row": lax.rem(row + delta + tiles, tiles)}

    links = [(step, delta) for step in (*range(1, regions), 0) for delta in (-1, 1, 0) if (step, delta) != (0, 0)]

    def when_there(delta, action):
        if delta == 0:
            action()
        else:
            pl.when(row > 0 if delta < 0 else row < tiles - 1)(action)

    loads = [pltpu.make_async_copy(flats, flats_v, load_sem.at[1]),
             pltpu.make_async_copy(proj.at[0], proj_v, load_sem.at[0]),
             pltpu.make_async_copy(starts, starts_s, load_sem.at[3])]
    lags = rows + 1
    table_load = pltpu.make_async_copy(table, table_v.at[pl.ds(0, lags * rows)], load_sem.at[4])
    weight_load = pltpu.make_async_copy(weights, weights_v, load_sem.at[2])
    for n in range(FLAT_CUTS):
        part = pl.ds(n * width // FLAT_CUTS, width // FLAT_CUTS)
        pltpu.make_async_copy(flats.at[:, part], flats_v.at[:, part], load_sem.at[1]).start()
    loads[1].start()
    loads[2].start()
    for d in range(lags):
        for n in range(TABLE_CUTS):
            part = pl.ds(n * width // TABLE_CUTS, width // TABLE_CUTS)
            pltpu.make_async_copy(table.at[pl.ds(d * rows, rows), part], table_v.at[pl.ds(d * cs, rows), part], load_sem.at[4]).start()
    weight_load.start()

    barrier = pltpu.get_barrier_semaphore()
    for step, delta in links:
        when_there(delta, lambda: pl.semaphore_signal(
            barrier, inc=1, device_id=peer(step, delta), device_id_type=pl.DeviceIdType.MESH))

    def slot(delta):
        return pl.ds((1 + delta) * rows, rows)

    zeros = jnp.zeros((angles, rows, shifts * LANES), jnp.bfloat16)
    pl.when(row == tiles - 1)(lambda: rbuf.at[:, slot(-1)].__setitem__(..., zeros))
    pl.when(row == 0)(lambda: rbuf.at[:, slot(1)].__setitem__(..., zeros))

    lane = lax.broadcasted_iota(jnp.int32, (rows, LANES), 1)
    sub = lax.broadcasted_iota(jnp.int32, (rows, LANES), 0)

    for copy in loads:
        copy.wait()

    pieces = [slice(b * LANES, (b + 1) * LANES) for b in range(blocks)]
    contrast = [1.0 - proj_v[:, p].astype(jnp.float32) / flats_v[:, p] for p in pieces]
    centre = jnp.sum(sum(contrast[:CENTRE]), axis=1, keepdims=True) / (CENTRE * LANES)
    for b, x in enumerate(contrast):
        xs[b] = x - centre
        xs[b + blocks] = x - centre

    table_load.wait()
    for g in range(regions):
        shifted = []
        for k in range(shifts):
            start = starts_s[me, g] + k * cs
            first = start // LANES
            rest = lax.rem(start, LANES)
            shift = lax.rem(LANES - rest, LANES)
            low = lane < LANES - rest
            turned = [pltpu.roll(xs[first + b], shift, 1) for b in range(blocks + 1)]
            shifted.append([jnp.where(low, turned[b], turned[b + 1]) for b in range(blocks)])
        for b in range(blocks):
            ys[g * shifts * rows:(g + 1) * shifts * rows, b * LANES:(b + 1) * LANES] = jnp.concatenate(
                [y[b] for y in shifted], axis=0).astype(jnp.bfloat16)

    cut = blocks // 2
    wide = lax.broadcasted_iota(jnp.int32, (2 * rows, LANES), 1)
    for d in range(0, lags, 2):
        pair = [e for e in (d, d + 1) if e < lags]
        turned = [pltpu.roll(jnp.concatenate([table_v[e * cs:e * cs + rows, p] for e in pair], axis=0).astype(jnp.float32), rows, 1)
                  for p in pieces]
        for b, p in enumerate(pieces):
            before = -turned[b - 1] if b in (0, cut) else turned[b - 1]
            value = jnp.where(wide[:len(pair) * rows] < rows, before, turned[b]).astype(jnp.bfloat16)
            for n, e in enumerate(pair):
                table_v[e * cs + rows:(e + 1) * cs, p] = value[n * rows:(n + 1) * rows]
    cut = cut * LANES
    near, far = (lax.dot_general(ys[:, part], table_v[:, part], (((1,), (1,)), ((), ())), preferred_element_type=jnp.float32)
                 for part in (slice(cut), slice(cut, width)))
    total = near - far
    total = jnp.concatenate([total, jnp.zeros((total.shape[0], LANES - cs), jnp.float32)], axis=1)

    lag = lane // cs
    up, down = lax.rem(sub + rows - lag, rows), lax.rem(sub + lag, rows)
    inside = [sub >= lag, (lag > 0) & (sub + lag < rows)]
    wrapped = [(sub < lag) | (lag == 0), sub + lag >= rows]
    parts = {0: inside,
             -1: [wrapped[0] & (up < half), wrapped[1] & (down < half)],
             1: [wrapped[0] & (up >= half), wrapped[1] & (down >= half)]}
    bits = [1 << n for n in range((rows - 1).bit_length())]
    for g in range(regions):
        for k in range(shifts):
            base = (g * shifts + k) * rows
            tile = total[base:base + rows, :LANES]
            last = total[base:base + rows, LANES:]
            ahead, back = tile, tile
            for bit in bits:
                turn = (lag & bit) > 0
                ahead = jnp.where(turn, pltpu.roll(ahead, bit, 0), ahead)
                back = jnp.where(turn, pltpu.roll(back, rows - bit, 0), back)
            edge = jnp.where(lag == 0, last, ahead)
            for delta, (first, second) in parts.items():
                value = jnp.where(first, edge if delta else ahead, 0.0) + jnp.where(second, back, 0.0)
                sbuf[(1 + delta) * regions + g, :, k * LANES:(k + 1) * LANES] = value.astype(jnp.bfloat16)

    sides = (row > 0).astype(jnp.int32) + (row < tiles - 1).astype(jnp.int32)
    pl.semaphore_wait(barrier, regions - 1 + sides * regions)

    for step, delta in links:
        to = peer(step, delta)
        low = (to["ang"] < regions // 2).astype(jnp.int32)
        final = (low if step == 1 else 0) + (1 - low if step == regions - 1 else 0)
        copy = pltpu.make_async_remote_copy(
            src_ref=sbuf.at[(1 + delta) * regions + to["ang"]], dst_ref=rbuf.at[me, slot(delta)],
            send_sem=send_sem, recv_sem=recv_sem.at[final],
            device_id=to, device_id_type=pl.DeviceIdType.MESH)
        when_there(delta, copy.start)
    weight_load.wait()
    rbuf[me, slot(0)] = sbuf[regions + me]

    inner = (row > 0) & (row < tiles - 1)
    turn = jnp.where(me < regions // 2, 1, regions - 1)

    def source(step):
        return lax.rem(me + step * turn, regions)

    def settled(full, short, sem, kind):
        def wait(count):
            units = sbuf.at[pl.ds(0, count)]
            kind(pltpu.make_async_remote_copy(
                src_ref=units, dst_ref=units, send_sem=send_sem, recv_sem=recv_sem.at[sem],
                device_id=peer(1, 0), device_id_type=pl.DeviceIdType.MESH))

        pl.when(inner)(lambda: wait(full))
        pl.when(jnp.logical_not(inner))(lambda: wait(short))

    def projected(steps):
        sums = []
        for half_pixels in range(2):
            pixels = pl.ds(half_pixels * (out.shape[1] // 2), out.shape[1] // 2)
            result = 0.0
            for step in steps:
                angle = source(step)
                w = jnp.concatenate(
                    [weights_v[angle, k * cs:(k + 1) * cs, pixels] for k in range(shifts) for _ in range(rows)], axis=0)
                result += jnp.dot(rbuf[angle], w, preferred_element_type=jnp.float32)
            sums.append(result[:rows] + result[rows:2 * rows] + result[2 * rows:])
        return jnp.concatenate(sums, axis=1)

    settled(3 * regions - 4, 2 * regions - 3, 0, lambda copy: copy.wait_recv())
    out[...] = projected(range(regions - 1))
    settled(3, 2, 1, lambda copy: copy.wait_recv())
    out[...] += projected([regions - 1])
    settled(3 * regions - 1, 2 * regions - 1, 0, lambda copy: copy.wait_send())


def body(projections, flats, block_start, bp_weights):
    _, rows, width = projections.shape
    angles, cb, pixels = bp_weights.shape
    regions, tiles = lax.axis_size("ang"), lax.axis_size("row")
    cs = LANES // rows
    shifts = cb // cs
    table = jnp.asarray(filter_table(rows + 2 * HALO, width, rows), jnp.bfloat16)
    lags = table.shape[0] // rows
    hbm = pl.BlockSpec(memory_space=pltpu.HBM)
    return pl.pallas_call(
        functools.partial(kernel, regions, tiles),
        name="fbp",
        out_shape=pltpu.VMEM((rows, pixels), jnp.float32),
        in_specs=[hbm, hbm, hbm, hbm, hbm],
        out_specs=pl.BlockSpec(memory_space=pltpu.VMEM),
        scratch_shapes=[
            pltpu.SMEM(block_start.shape, jnp.int32),
            pltpu.VMEM((rows, width), jnp.bfloat16),
            pltpu.VMEM((rows, width), jnp.float32),
            pltpu.VMEM((lags * cs, width), jnp.bfloat16),
            pltpu.VMEM(bp_weights.shape, jnp.bfloat16),
            pltpu.VMEM((2 * width // LANES, rows, LANES), jnp.float32),
            pltpu.VMEM((regions * shifts * rows, width), jnp.bfloat16),
            pltpu.VMEM((3 * regions, rows, shifts * LANES), jnp.bfloat16),
            pltpu.VMEM((angles, 3 * rows, shifts * LANES), jnp.bfloat16),
            pltpu.SemaphoreType.DMA((5,)),
            pltpu.SemaphoreType.DMA,
            pltpu.SemaphoreType.DMA((2,)),
        ],
        compiler_params=pltpu.CompilerParams(collective_id=0, has_side_effects=True, vmem_limit_bytes=65000000),
    )(block_start, projections, flats, table, bp_weights)


def solution(mesh):
    placed = (P(("scan", "ang"), "row", None), P(("scan", "row"), None), P(), P(None, None, "ang"))
    return jax.shard_map(
        body, mesh=mesh, in_specs=placed, out_specs=P(("scan", "row"), "ang"), check_vma=False
    )
```

```python
import functools

import jax
import jax.numpy as jnp
import numpy as np
from jax import lax
from jax.experimental import pallas as pl
from jax.experimental.pallas import tpu as pltpu
from jax.sharding import PartitionSpec as P

HALO = 4
LANES = 128
FLAT_CUTS = 2
TABLE_CUTS = 2
CENTRE = 4
paganin_beta = 8.0
ramp_gain = 320.0


def filter_table(tile_rows, width, columns):
    u = np.arange(tile_rows, dtype=np.float64)
    v = np.arange(width, dtype=np.float64)
    lam = (4.0 * np.sin(np.pi * u / tile_rows) ** 2)[:, None] + (4.0 * np.sin(np.pi * v / width) ** 2)[None, :]
    folded = np.minimum(v, width - v)
    ramp = ramp_gain * (folded / width) * (0.5 + 0.5 * np.cos(2.0 * np.pi * folded / width))
    taps = np.real(np.fft.ifft2(ramp[None, :] / (1.0 + paganin_beta * lam)))
    lags = tile_rows // 2 + 1
    place = (np.arange(columns)[:, None] - np.arange(width)[None, :]) % width
    sign = np.where(np.arange(width) < width // LANES // 2 * LANES, 1.0, -1.0)
    return taps[:lags][:, place].reshape(lags * columns, width) * sign


def kernel(regions, tiles, starts, proj, flats, table, weights, out,
           starts_s, proj_v, flats_v, table_v, weights_v, xs, ys, sbuf, rbuf,
           load_sem, send_sem, recv_sem):
    rows, width = flats.shape
    blocks = width // LANES
    angles, cb, _ = weights.shape
    half = rows // 2
    cs = LANES // (2 * rows)
    shifts = cb // cs
    pairs = shifts // 2
    lags = rows + 1
    order = [(0, 0), (1, 0), *[(0, d) for d in range(1, rows)], (1, rows - 1), *[(1, d) for d in range(1, rows - 1)]]
    me = lax.axis_index("ang")
    row = lax.axis_index("row")

    def peer(step, delta):
        return {"ang": lax.rem(me + step, regions), "row": lax.rem(row + delta + tiles, tiles)}

    links = [(step, delta) for step in (*range(1, regions), 0) for delta in (-1, 1, 0) if (step, delta) != (0, 0)]

    def when_there(delta, action):
        if delta == 0:
            action()
        else:
            pl.when(row > 0 if delta < 0 else row < tiles - 1)(action)

    loads = [pltpu.make_async_copy(flats, flats_v, load_sem.at[1]),
             pltpu.make_async_copy(proj.at[0], proj_v, load_sem.at[0]),
             pltpu.make_async_copy(starts, starts_s, load_sem.at[3])]
    table_load = pltpu.make_async_copy(table, table_v, load_sem.at[4])
    weight_load = pltpu.make_async_copy(weights, weights_v, load_sem.at[2])
    for n in range(FLAT_CUTS):
        part = pl.ds(n * width // FLAT_CUTS, width // FLAT_CUTS)
        pltpu.make_async_copy(flats.at[:, part], flats_v.at[:, part], load_sem.at[1]).start()
    loads[1].start()
    loads[2].start()
    for d in range(lags):
        for n in range(TABLE_CUTS):
            part = pl.ds(n * width // TABLE_CUTS, width // TABLE_CUTS)
            pltpu.make_async_copy(table.at[pl.ds(d * cs, cs), part], table_v.at[pl.ds(d * cs, cs), part], load_sem.at[4]).start()
    weight_load.start()

    barrier = pltpu.get_barrier_semaphore()
    for step, delta in links:
        when_there(delta, lambda: pl.semaphore_signal(
            barrier, inc=1, device_id=peer(step, delta), device_id_type=pl.DeviceIdType.MESH))

    def slot(delta):
        return pl.ds((1 + delta) * rows, rows)

    zeros = jnp.zeros((angles, rows, pairs * LANES), jnp.bfloat16)
    pl.when(row == tiles - 1)(lambda: rbuf.at[:, slot(-1)].__setitem__(..., zeros))
    pl.when(row == 0)(lambda: rbuf.at[:, slot(1)].__setitem__(..., zeros))

    lane = lax.broadcasted_iota(jnp.int32, (rows, LANES), 1)
    sub = lax.broadcasted_iota(jnp.int32, (rows, LANES), 0)

    for copy in loads:
        copy.wait()

    pieces = [slice(b * LANES, (b + 1) * LANES) for b in range(blocks)]
    contrast = [1.0 - proj_v[:, p].astype(jnp.float32) / flats_v[:, p] for p in pieces]
    centre = jnp.sum(sum(contrast[:CENTRE]), axis=1, keepdims=True) / (CENTRE * LANES)
    for b, x in enumerate(contrast):
        xs[b] = x - centre
        xs[b + blocks] = x - centre

    spot = lane // cs
    lag = jnp.where(spot < 2, 0, jnp.where(spot < rows, spot - 1, jnp.where(spot < rows + 2, rows - 1, spot - rows - 1)))
    odd = (spot == 1) | (spot > rows)
    up, down = lax.rem(sub + rows - lag, rows), lax.rem(sub + lag, rows)
    inside = [sub >= lag, (lag > 0) & (sub + lag < rows)]
    wrapped = [(sub < lag) | (lag == 0), sub + lag >= rows]
    parts = {-1: [wrapped[0] & (up < half), wrapped[1] & (down < half)],
             1: [wrapped[0] & (up >= half), wrapped[1] & (down >= half)],
             0: inside}
    bits = [1 << n for n in range((rows - 1).bit_length())]
    def filtered(group):
        deep = shifts * rows
        for region in group:
            shifted = []
            for k in range(shifts):
                start = starts_s[me, region] + k * cs
                first = start // LANES
                rest = lax.rem(start, LANES)
                shift = lax.rem(LANES - rest, LANES)
                low = lane < LANES - rest
                turned = [pltpu.roll(xs[first + b], shift, 1) for b in range(blocks + 1)]
                shifted.append([jnp.where(low, turned[b], turned[b + 1]) for b in range(blocks)])
            for b in range(blocks):
                place = region * deep
                ys[place:place + deep, pieces[b]] = jnp.concatenate(
                    [y[b] for y in shifted], axis=0).astype(jnp.bfloat16)
        cut = blocks // 2 * LANES
        begin = group[0] * deep
        end = begin + len(group) * deep
        near, far = (lax.dot_general(
            ys[begin:end, part], jnp.concatenate([table_v[d * cs:(d + 1) * cs, part] for _, d in [*order, (0, rows), (1, rows)]], axis=0),
            (((1,), (1,)), ((), ())), preferred_element_type=jnp.float32) for part in (slice(cut), slice(cut, width)))
        total = near - far
        total = jnp.concatenate([total, jnp.zeros((total.shape[0], LANES - 2 * cs), jnp.float32)], axis=1)
        for n, region in enumerate(group):
            for k in range(pairs):
                base = n * deep + k * 2 * rows
                even_rows, odd_rows = total[base:base + rows], total[base + rows:base + 2 * rows]
                tile = jnp.where(odd, odd_rows[:, :LANES], even_rows[:, :LANES])
                last = jnp.where(odd, odd_rows[:, LANES:], even_rows[:, LANES:])
                ahead, back = tile, tile
                for bit in bits:
                    turn = (lag & bit) > 0
                    ahead = jnp.where(turn, pltpu.roll(ahead, bit, 0), ahead)
                    back = jnp.where(turn, pltpu.roll(back, rows - bit, 0), back)
                edge = jnp.where(lag == 0, last, ahead)
                for delta, (first, second) in parts.items():
                    value = jnp.where(first, edge if delta else ahead, 0.0) + jnp.where(second, back, 0.0)
                    sbuf[(1 + delta) * regions + region, :, k * LANES:(k + 1) * LANES] = value.astype(jnp.bfloat16)

    def send(group):
        for region in group:
            last = (region + (regions - 1 if region < regions // 2 else 1)) % regions
            final = (me == last).astype(jnp.int32)
            for delta in (-1, 1, 0):
                copy = pltpu.make_async_remote_copy(
                    src_ref=sbuf.at[(1 + delta) * regions + region], dst_ref=rbuf.at[me, slot(delta)],
                    send_sem=send_sem, recv_sem=recv_sem.at[final],
                    device_id={"ang": region, "row": lax.rem(row + delta + tiles, tiles)},
                    device_id_type=pl.DeviceIdType.MESH)
                if delta == 0:
                    pl.when(me != region)(copy.start)
                else:
                    when_there(delta, copy.start)

    table_load.wait()
    filtered([0])
    sides = (row > 0).astype(jnp.int32) + (row < tiles - 1).astype(jnp.int32)
    pl.semaphore_wait(barrier, regions - 1 + sides * regions)
    send([0])
    filtered([*range(1, regions)])
    send([*range(1, regions)])
    weight_load.wait()
    rbuf[me, slot(0)] = sbuf[regions + me]

    inner = (row > 0) & (row < tiles - 1)
    turn = jnp.where(me < regions // 2, 1, regions - 1)

    def source(step):
        return lax.rem(me + step * turn, regions)

    def settled(full, short, sem, kind):
        def wait(count):
            units = sbuf.at[pl.ds(0, count)]
            kind(pltpu.make_async_remote_copy(
                src_ref=units, dst_ref=units, send_sem=send_sem, recv_sem=recv_sem.at[sem],
                device_id=peer(1, 0), device_id_type=pl.DeviceIdType.MESH))

        pl.when(inner)(lambda: wait(full))
        pl.when(jnp.logical_not(inner))(lambda: wait(short))

    def projected(steps):
        sums = []
        for half_pixels in range(2):
            pixels = pl.ds(half_pixels * (out.shape[1] // 2), out.shape[1] // 2)
            result = 0.0
            for step in steps:
                angle = source(step)
                w = jnp.concatenate(
                    [weights_v[angle, (2 * k + side) * cs:(2 * k + side + 1) * cs, pixels]
                     for k in range(pairs) for side, _ in order], axis=0)
                result += jnp.dot(rbuf[angle], w, preferred_element_type=jnp.float32)
            sums.append(result[:rows] + result[rows:2 * rows] + result[2 * rows:])
        return jnp.concatenate(sums, axis=1)

    settled(3 * regions - 4, 2 * regions - 3, 0, lambda copy: copy.wait_recv())
    out[...] = projected(range(regions - 1))
    settled(3, 2, 1, lambda copy: copy.wait_recv())
    out[...] += projected([regions - 1])
    settled(3 * regions - 1, 2 * regions - 1, 0, lambda copy: copy.wait_send())


def body(projections, flats, block_start, bp_weights):
    _, rows, width = projections.shape
    angles, cb, pixels = bp_weights.shape
    regions, tiles = lax.axis_size("ang"), lax.axis_size("row")
    cs = LANES // (2 * rows)
    pairs = cb // cs // 2
    table = jnp.asarray(filter_table(rows + 2 * HALO, width, cs), jnp.bfloat16)
    hbm = pl.BlockSpec(memory_space=pltpu.HBM)
    return pl.pallas_call(
        functools.partial(kernel, regions, tiles),
        name="fbp",
        out_shape=pltpu.VMEM((rows, pixels), jnp.float32),
        in_specs=[hbm, hbm, hbm, hbm, hbm],
        out_specs=pl.BlockSpec(memory_space=pltpu.VMEM),
        scratch_shapes=[
            pltpu.SMEM(block_start.shape, jnp.int32),
            pltpu.VMEM((rows, width), jnp.bfloat16),
            pltpu.VMEM((rows, width), jnp.float32),
            pltpu.VMEM(table.shape, jnp.bfloat16),
            pltpu.VMEM(bp_weights.shape, jnp.bfloat16),
            pltpu.VMEM((2 * width // LANES, rows, LANES), jnp.float32),
            pltpu.VMEM((regions * (cb // cs) * rows, width), jnp.bfloat16),
            pltpu.VMEM((3 * regions, rows, pairs * LANES), jnp.bfloat16),
            pltpu.VMEM((angles, 3 * rows, pairs * LANES), jnp.bfloat16),
            pltpu.SemaphoreType.DMA((5,)),
            pltpu.SemaphoreType.DMA,
            pltpu.SemaphoreType.DMA((2,)),
        ],
        compiler_params=pltpu.CompilerParams(collective_id=0, has_side_effects=True, vmem_limit_bytes=65000000),
    )(block_start, projections, flats, table, bp_weights)


def solution(mesh):
    placed = (P(("scan", "ang"), "row", None), P(("scan", "row"), None), P(), P(None, None, "ang"))
    return jax.shard_map(
        body, mesh=mesh, in_specs=placed, out_specs=P(("scan", "row"), "ang"), check_vma=False
    )
```

```python
import functools

import jax
import jax.numpy as jnp
import numpy as np
from jax import lax
from jax.experimental import pallas as pl
from jax.experimental.pallas import tpu as pltpu
from jax.sharding import PartitionSpec as P

HALO = 4
LANES = 128
FLAT_CUTS = 2
TABLE_CUTS = 2
CENTRE = 4
paganin_beta = 8.0
ramp_gain = 320.0


def filter_table(tile_rows, width, columns):
    u = np.arange(tile_rows, dtype=np.float64)
    v = np.arange(width, dtype=np.float64)
    lam = (4.0 * np.sin(np.pi * u / tile_rows) ** 2)[:, None] + (4.0 * np.sin(np.pi * v / width) ** 2)[None, :]
    folded = np.minimum(v, width - v)
    ramp = ramp_gain * (folded / width) * (0.5 + 0.5 * np.cos(2.0 * np.pi * folded / width))
    taps = np.real(np.fft.ifft2(ramp[None, :] / (1.0 + paganin_beta * lam)))
    lags = tile_rows // 2 + 1
    place = (np.arange(columns)[:, None] - np.arange(width)[None, :]) % width
    sign = np.where(np.arange(width) < width // LANES // 2 * LANES, 1.0, -1.0)
    return taps[:lags][:, place].reshape(lags * columns, width) * sign


def kernel(regions, tiles, starts, proj, flats, table, weights, out,
           starts_s, proj_v, flats_v, table_v, weights_v, xs, ys, sbuf, rbuf,
           load_sem, send_sem, recv_sem):
    rows, width = flats.shape
    blocks = width // LANES
    angles, cb, _ = weights.shape
    half = rows // 2
    cs = LANES // (2 * rows)
    shifts = cb // cs
    pairs = shifts // 2
    lags = rows + 1
    order = [(0, 0), (1, 0), *[(0, d) for d in range(1, rows)], (1, rows - 1), *[(1, d) for d in range(1, rows - 1)]]
    me = lax.axis_index("ang")
    row = lax.axis_index("row")

    def peer(step, delta):
        return {"ang": lax.rem(me + step, regions), "row": lax.rem(row + delta + tiles, tiles)}

    links = [(step, delta) for step in (*range(1, regions), 0) for delta in (-1, 1, 0) if (step, delta) != (0, 0)]

    def when_there(delta, action):
        if delta == 0:
            action()
        else:
            pl.when(row > 0 if delta < 0 else row < tiles - 1)(action)

    start_load = pltpu.make_async_copy(starts, starts_s, load_sem.at[3])
    table_load = pltpu.make_async_copy(table, table_v, load_sem.at[4])
    weight_load = pltpu.make_async_copy(weights, weights_v, load_sem.at[2])

    def load_columns(begin, end, cuts, sem):
        for n in range(cuts):
            part = pl.ds((begin + n * (end - begin) // cuts) * LANES, (end - begin) // cuts * LANES)
            pltpu.make_async_copy(flats.at[:, part], flats_v.at[:, part], sem).start()
        part = pl.ds(begin * LANES, (end - begin) * LANES)
        pltpu.make_async_copy(proj.at[0, :, part], proj_v.at[:, part], sem).start()

    def columns_loaded(count, sem):
        both = xs.at[pl.ds(0, count * 3 // 2)]
        pltpu.make_async_copy(both, both, sem).wait()

    load_columns(0, CENTRE, 1, load_sem.at[0])
    load_columns(CENTRE, blocks, FLAT_CUTS, load_sem.at[1])
    start_load.start()
    for d in range(lags):
        for n in range(TABLE_CUTS):
            part = pl.ds(n * width // TABLE_CUTS, width // TABLE_CUTS)
            pltpu.make_async_copy(table.at[pl.ds(d * cs, cs), part], table_v.at[pl.ds(d * cs, cs), part], load_sem.at[4]).start()
    weight_load.start()

    barrier = pltpu.get_barrier_semaphore()
    for step, delta in links:
        when_there(delta, lambda: pl.semaphore_signal(
            barrier, inc=1, device_id=peer(step, delta), device_id_type=pl.DeviceIdType.MESH))

    def slot(delta):
        return pl.ds((1 + delta) * rows, rows)

    zeros = jnp.zeros((angles, rows, pairs * LANES), jnp.bfloat16)
    pl.when(row == tiles - 1)(lambda: rbuf.at[:, slot(-1)].__setitem__(..., zeros))
    pl.when(row == 0)(lambda: rbuf.at[:, slot(1)].__setitem__(..., zeros))

    lane = lax.broadcasted_iota(jnp.int32, (rows, LANES), 1)
    sub = lax.broadcasted_iota(jnp.int32, (rows, LANES), 0)

    pieces = [slice(b * LANES, (b + 1) * LANES) for b in range(blocks)]

    def contrast_of(p):
        return 1.0 - proj_v[:, p].astype(jnp.float32) / flats_v[:, p]

    columns_loaded(CENTRE, load_sem.at[0])
    contrast = [contrast_of(p) for p in pieces[:CENTRE]]
    centre = jnp.sum(sum(contrast), axis=1, keepdims=True) / (CENTRE * LANES)
    columns_loaded(blocks - CENTRE, load_sem.at[1])
    start_load.wait()

    contrast += [contrast_of(p) for p in pieces[CENTRE:]]
    for b, x in enumerate(contrast):
        xs[b] = x - centre
        xs[b + blocks] = x - centre

    spot = lane // cs
    lag = jnp.where(spot < 2, 0, jnp.where(spot < rows, spot - 1, jnp.where(spot < rows + 2, rows - 1, spot - rows - 1)))
    odd = (spot == 1) | (spot > rows)
    up, down = lax.rem(sub + rows - lag, rows), lax.rem(sub + lag, rows)
    inside = [sub >= lag, (lag > 0) & (sub + lag < rows)]
    wrapped = [(sub < lag) | (lag == 0), sub + lag >= rows]
    parts = {-1: [wrapped[0] & (up < half), wrapped[1] & (down < half)],
             1: [wrapped[0] & (up >= half), wrapped[1] & (down >= half)],
             0: inside}
    bits = [1 << n for n in range((rows - 1).bit_length())]
    deep = shifts * rows

    def shifted_rows(group):
        for region in group:
            shifted = []
            for k in range(shifts):
                start = starts_s[me, region] + k * cs
                first = start // LANES
                rest = lax.rem(start, LANES)
                shift = lax.rem(LANES - rest, LANES)
                low = lane < LANES - rest
                turned = [pltpu.roll(xs[first + b], shift, 1) for b in range(blocks + 1)]
                shifted.append([jnp.where(low, turned[b], turned[b + 1]) for b in range(blocks)])
            for b in range(blocks):
                place = region * deep
                ys[place:place + deep, pieces[b]] = jnp.concatenate(
                    [y[b] for y in shifted], axis=0).astype(jnp.bfloat16)

    def filtered(group):
        cut = blocks // 2 * LANES
        begin = group[0] * deep
        end = begin + len(group) * deep
        near, far = (lax.dot_general(
            ys[begin:end, part], jnp.concatenate([table_v[d * cs:(d + 1) * cs, part] for _, d in [*order, (0, rows), (1, rows)]], axis=0),
            (((1,), (1,)), ((), ())), preferred_element_type=jnp.float32) for part in (slice(cut), slice(cut, width)))
        total = near - far
        total = jnp.concatenate([total, jnp.zeros((total.shape[0], LANES - 2 * cs), jnp.float32)], axis=1)
        for n, region in enumerate(group):
            for k in range(pairs):
                base = n * deep + k * 2 * rows
                even_rows, odd_rows = total[base:base + rows], total[base + rows:base + 2 * rows]
                tile = jnp.where(odd, odd_rows[:, :LANES], even_rows[:, :LANES])
                last = jnp.where(odd, odd_rows[:, LANES:], even_rows[:, LANES:])
                ahead, back = tile, tile
                for bit in bits:
                    turn = (lag & bit) > 0
                    ahead = jnp.where(turn, pltpu.roll(ahead, bit, 0), ahead)
                    back = jnp.where(turn, pltpu.roll(back, rows - bit, 0), back)
                edge = jnp.where(lag == 0, last, ahead)
                for delta, (first, second) in parts.items():
                    value = jnp.where(first, edge if delta else ahead, 0.0) + jnp.where(second, back, 0.0)
                    sbuf[(1 + delta) * regions + region, :, k * LANES:(k + 1) * LANES] = value.astype(jnp.bfloat16)

    def send(group):
        for region in group:
            last = (region + (regions - 1 if region < regions // 2 else 1)) % regions
            final = (me == last).astype(jnp.int32)
            for delta in (-1, 1, 0):
                copy = pltpu.make_async_remote_copy(
                    src_ref=sbuf.at[(1 + delta) * regions + region], dst_ref=rbuf.at[me, slot(delta)],
                    send_sem=send_sem, recv_sem=recv_sem.at[final],
                    device_id={"ang": region, "row": lax.rem(row + delta + tiles, tiles)},
                    device_id_type=pl.DeviceIdType.MESH)
                if delta == 0:
                    pl.when(me != region)(copy.start)
                else:
                    when_there(delta, copy.start)

    shifted_rows([0])
    table_load.wait()
    filtered([0])
    sides = (row > 0).astype(jnp.int32) + (row < tiles - 1).astype(jnp.int32)
    pl.semaphore_wait(barrier, regions - 1 + sides * regions)
    send([0])
    shifted_rows([*range(1, regions)])
    filtered([*range(1, regions)])
    send([*range(1, regions)])
    weight_load.wait()
    rbuf[me, slot(0)] = sbuf[regions + me]

    inner = (row > 0) & (row < tiles - 1)
    turn = jnp.where(me < regions // 2, 1, regions - 1)

    def source(step):
        return lax.rem(me + step * turn, regions)

    def settled(full, short, sem, kind):
        def wait(count):
            units = sbuf.at[pl.ds(0, count)]
            kind(pltpu.make_async_remote_copy(
                src_ref=units, dst_ref=units, send_sem=send_sem, recv_sem=recv_sem.at[sem],
                device_id=peer(1, 0), device_id_type=pl.DeviceIdType.MESH))

        pl.when(inner)(lambda: wait(full))
        pl.when(jnp.logical_not(inner))(lambda: wait(short))

    def projected(steps):
        sums = []
        for half_pixels in range(2):
            pixels = pl.ds(half_pixels * (out.shape[1] // 2), out.shape[1] // 2)
            result = 0.0
            for step in steps:
                angle = source(step)
                w = jnp.concatenate(
                    [weights_v[angle, (2 * k + side) * cs:(2 * k + side + 1) * cs, pixels]
                     for k in range(pairs) for side, _ in order], axis=0)
                result += jnp.dot(rbuf[angle], w, preferred_element_type=jnp.float32)
            sums.append(result[:rows] + result[rows:2 * rows] + result[2 * rows:])
        return jnp.concatenate(sums, axis=1)

    settled(3 * regions - 4, 2 * regions - 3, 0, lambda copy: copy.wait_recv())
    out[...] = projected(range(regions - 1))
    settled(3, 2, 1, lambda copy: copy.wait_recv())
    out[...] += projected([regions - 1])
    settled(3 * regions - 1, 2 * regions - 1, 0, lambda copy: copy.wait_send())


def body(projections, flats, block_start, bp_weights):
    _, rows, width = projections.shape
    angles, cb, pixels = bp_weights.shape
    regions, tiles = lax.axis_size("ang"), lax.axis_size("row")
    cs = LANES // (2 * rows)
    pairs = cb // cs // 2
    table = jnp.asarray(filter_table(rows + 2 * HALO, width, cs), jnp.bfloat16)
    hbm = pl.BlockSpec(memory_space=pltpu.HBM)
    return pl.pallas_call(
        functools.partial(kernel, regions, tiles),
        name="fbp",
        out_shape=pltpu.VMEM((rows, pixels), jnp.float32),
        in_specs=[hbm, hbm, hbm, hbm, hbm],
        out_specs=pl.BlockSpec(memory_space=pltpu.VMEM),
        scratch_shapes=[
            pltpu.SMEM(block_start.shape, jnp.int32),
            pltpu.VMEM((rows, width), jnp.bfloat16),
            pltpu.VMEM((rows, width), jnp.float32),
            pltpu.VMEM(table.shape, jnp.bfloat16),
            pltpu.VMEM(bp_weights.shape, jnp.bfloat16),
            pltpu.VMEM((2 * width // LANES, rows, LANES), jnp.float32),
            pltpu.VMEM((regions * (cb // cs) * rows, width), jnp.bfloat16),
            pltpu.VMEM((3 * regions, rows, pairs * LANES), jnp.bfloat16),
            pltpu.VMEM((angles, 3 * rows, pairs * LANES), jnp.bfloat16),
            pltpu.SemaphoreType.DMA((5,)),
            pltpu.SemaphoreType.DMA,
            pltpu.SemaphoreType.DMA((2,)),
        ],
        compiler_params=pltpu.CompilerParams(collective_id=0, has_side_effects=True, vmem_limit_bytes=65000000),
    )(block_start, projections, flats, table, bp_weights)


def solution(mesh):
    placed = (P(("scan", "ang"), "row", None), P(("scan", "row"), None), P(), P(None, None, "ang"))
    return jax.shard_map(
        body, mesh=mesh, in_specs=placed, out_specs=P(("scan", "row"), "ang"), check_vma=False
    )
```

```python
import functools

import jax
import jax.numpy as jnp
import numpy as np
from jax import lax
from jax.experimental import pallas as pl
from jax.experimental.pallas import tpu as pltpu
from jax.sharding import PartitionSpec as P

HALO = 4
LANES = 128
FLAT_CUTS = 2
TABLE_CUTS = 2
CENTRE = 4
paganin_beta = 8.0
ramp_gain = 320.0


def filter_table(tile_rows, width, columns):
    u = np.arange(tile_rows, dtype=np.float64)
    v = np.arange(width, dtype=np.float64)
    lam = (4.0 * np.sin(np.pi * u / tile_rows) ** 2)[:, None] + (4.0 * np.sin(np.pi * v / width) ** 2)[None, :]
    folded = np.minimum(v, width - v)
    ramp = ramp_gain * (folded / width) * (0.5 + 0.5 * np.cos(2.0 * np.pi * folded / width))
    taps = np.real(np.fft.ifft2(ramp[None, :] / (1.0 + paganin_beta * lam)))
    lags = tile_rows // 2 + 1
    place = (np.arange(columns)[:, None] - np.arange(width)[None, :]) % width
    sign = np.where(np.arange(width) < width // LANES // 2 * LANES, 1.0, -1.0)
    return taps[:lags][:, place].reshape(lags * columns, width) * sign


def kernel(regions, tiles, starts, proj, flats, table, weights, out,
           starts_s, proj_v, flats_v, table_v, weights_v, xs, ys, sbuf, rbuf,
           load_sem, done_sem):
    rows, width = flats.shape
    blocks = width // LANES
    angles, cb, _ = weights.shape
    half = rows // 2
    cs = LANES // (2 * rows)
    shifts = cb // cs
    pairs = shifts // 2
    lags = rows + 1
    order = [(0, 0), (1, 0), *[(0, d) for d in range(1, rows)], (1, rows - 1), *[(1, d) for d in range(1, rows - 1)]]
    me = lax.axis_index("ang")
    row = lax.axis_index("row")

    def peer(step, delta):
        return {"ang": lax.rem(me + step, regions), "row": lax.rem(row + delta + tiles, tiles)}

    def when_there(delta, action):
        if delta == 0:
            action()
        else:
            pl.when(row > 0 if delta < 0 else row < tiles - 1)(action)

    start_load = pltpu.make_async_copy(starts, starts_s, load_sem.at[2])
    table_load = pltpu.make_async_copy(table, table_v, load_sem.at[3])
    weight_load = pltpu.make_async_copy(weights, weights_v, done_sem.at[0])

    def load_columns(begin, end, cuts, sem):
        for n in range(cuts):
            part = pl.ds((begin + n * (end - begin) // cuts) * LANES, (end - begin) // cuts * LANES)
            pltpu.make_async_copy(flats.at[:, part], flats_v.at[:, part], sem).start()
        part = pl.ds(begin * LANES, (end - begin) * LANES)
        pltpu.make_async_copy(proj.at[0, :, part], proj_v.at[:, part], sem).start()

    def columns_loaded(count, sem):
        both = xs.at[pl.ds(0, count * 3 // 2)]
        pltpu.make_async_copy(both, both, sem).wait()

    load_columns(0, CENTRE, 1, load_sem.at[0])
    load_columns(CENTRE, blocks, FLAT_CUTS, load_sem.at[1])
    start_load.start()
    for d in range(lags):
        for n in range(TABLE_CUTS):
            part = pl.ds(n * width // TABLE_CUTS, width // TABLE_CUTS)
            pltpu.make_async_copy(table.at[pl.ds(d * cs, cs), part], table_v.at[pl.ds(d * cs, cs), part], load_sem.at[3]).start()
    weight_load.start()

    barrier = pltpu.get_barrier_semaphore()
    def greet(delta):
        for step in range(regions):
            if (step, delta) != (0, 0):
                pl.semaphore_signal(barrier, inc=1, device_id=peer(step, delta), device_id_type=pl.DeviceIdType.MESH)

    for delta in (-1, 0, 1):
        when_there(delta, lambda: greet(delta))

    def slot(delta):
        return pl.ds((1 + delta) * rows, rows)

    zeros = jnp.zeros((angles, rows, pairs * LANES), jnp.bfloat16)
    pl.when(row == tiles - 1)(lambda: rbuf.at[:, slot(-1)].__setitem__(..., zeros))
    pl.when(row == 0)(lambda: rbuf.at[:, slot(1)].__setitem__(..., zeros))

    lane = lax.broadcasted_iota(jnp.int32, (rows, LANES), 1)
    sub = lax.broadcasted_iota(jnp.int32, (rows, LANES), 0)

    pieces = [slice(b * LANES, (b + 1) * LANES) for b in range(blocks)]

    def contrast_of(p):
        return 1.0 - proj_v[:, p].astype(jnp.float32) / flats_v[:, p]

    columns_loaded(CENTRE, load_sem.at[0])
    contrast = [contrast_of(p) for p in pieces[:CENTRE]]
    centre = jnp.sum(sum(contrast), axis=1, keepdims=True) / (CENTRE * LANES)
    columns_loaded(blocks - CENTRE, load_sem.at[1])
    start_load.wait()

    contrast += [contrast_of(p) for p in pieces[CENTRE:]]
    for b, x in enumerate(contrast):
        xs[b] = x - centre
        xs[b + blocks] = x - centre

    spot = lane // cs
    lag = jnp.where(spot < 2, 0, jnp.where(spot < rows, spot - 1, jnp.where(spot < rows + 2, rows - 1, spot - rows - 1)))
    odd = (spot == 1) | (spot > rows)
    up, down = lax.rem(sub + rows - lag, rows), lax.rem(sub + lag, rows)
    inside = [sub >= lag, (lag > 0) & (sub + lag < rows)]
    wrapped = [(sub < lag) | (lag == 0), sub + lag >= rows]
    parts = {-1: [wrapped[0] & (up < half), wrapped[1] & (down < half)],
             1: [wrapped[0] & (up >= half), wrapped[1] & (down >= half)],
             0: inside}
    bits = [1 << n for n in range((rows - 1).bit_length())]
    deep = shifts * rows

    def shifted_rows(group):
        for region in group:
            shifted = []
            for k in range(shifts):
                start = starts_s[me, region] + k * cs
                first = start // LANES
                rest = lax.rem(start, LANES)
                shift = lax.rem(LANES - rest, LANES)
                low = lane < LANES - rest
                turned = [pltpu.roll(xs[first + b], shift, 1) for b in range(blocks + 1)]
                shifted.append([jnp.where(low, turned[b], turned[b + 1]) for b in range(blocks)])
            for b in range(blocks):
                place = region * deep
                ys[place:place + deep, pieces[b]] = jnp.concatenate(
                    [y[b] for y in shifted], axis=0).astype(jnp.bfloat16)

    def filtered(group):
        cut = blocks // 2 * LANES
        begin = group[0] * deep
        end = begin + len(group) * deep
        near, far = (lax.dot_general(
            ys[begin:end, part], jnp.concatenate([table_v[d * cs:(d + 1) * cs, part] for _, d in [*order, (0, rows), (1, rows)]], axis=0),
            (((1,), (1,)), ((), ())), preferred_element_type=jnp.float32) for part in (slice(cut), slice(cut, width)))
        total = near - far
        total = jnp.concatenate([total, jnp.zeros((total.shape[0], LANES - 2 * cs), jnp.float32)], axis=1)
        for n, region in enumerate(group):
            for k in range(pairs):
                base = n * deep + k * 2 * rows
                even_rows, odd_rows = total[base:base + rows], total[base + rows:base + 2 * rows]
                tile = jnp.where(odd, odd_rows[:, :LANES], even_rows[:, :LANES])
                last = jnp.where(odd, odd_rows[:, LANES:], even_rows[:, LANES:])
                ahead, back = tile, tile
                for bit in bits:
                    turn = (lag & bit) > 0
                    ahead = jnp.where(turn, pltpu.roll(ahead, bit, 0), ahead)
                    back = jnp.where(turn, pltpu.roll(back, rows - bit, 0), back)
                edge = jnp.where(lag == 0, last, ahead)
                for delta, (first, second) in parts.items():
                    value = jnp.where(first, edge if delta else ahead, 0.0) + jnp.where(second, back, 0.0)
                    sbuf[(1 + delta) * regions + region, :, k * LANES:(k + 1) * LANES] = value.astype(jnp.bfloat16)

    def send(group):
        for region in group:
            last = (region + (regions - 1 if region < regions // 2 else 1)) % regions
            final = (me == last).astype(jnp.int32)
            for delta in (-1, 1, 0):
                copy = pltpu.make_async_remote_copy(
                    src_ref=sbuf.at[(1 + delta) * regions + region], dst_ref=rbuf.at[me, slot(delta)],
                    send_sem=done_sem.at[0], recv_sem=done_sem.at[final],
                    device_id={"ang": region, "row": lax.rem(row + delta + tiles, tiles)},
                    device_id_type=pl.DeviceIdType.MESH)
                if delta == 0:
                    pl.when(me != region)(copy.start)
                else:
                    when_there(delta, copy.start)

    shifted_rows([0])
    table_load.wait()
    filtered([0])
    sides = (row > 0).astype(jnp.int32) + (row < tiles - 1).astype(jnp.int32)
    pl.semaphore_wait(barrier, regions - 1 + sides * regions)
    send([0])
    shifted_rows([*range(1, regions)])
    filtered([*range(1, regions)])
    send([*range(1, regions)])
    rbuf[me, slot(0)] = sbuf[regions + me]

    inner = (row > 0) & (row < tiles - 1)
    turn = jnp.where(me < regions // 2, 1, regions - 1)

    def source(step):
        return lax.rem(me + step * turn, regions)

    def settled(full, short, sem):
        def wait(count):
            units = sbuf.at[pl.ds(0, count)]
            pltpu.make_async_copy(units, units, done_sem.at[sem]).wait()

        pl.when(inner)(lambda: wait(full))
        pl.when(jnp.logical_not(inner))(lambda: wait(short))

    def projected(steps):
        sums = []
        for half_pixels in range(2):
            pixels = pl.ds(half_pixels * (out.shape[1] // 2), out.shape[1] // 2)
            result = 0.0
            for step in steps:
                angle = source(step)
                w = jnp.concatenate(
                    [weights_v[angle, (2 * k + side) * cs:(2 * k + side + 1) * cs, pixels]
                     for k in range(pairs) for side, _ in order], axis=0)
                result += jnp.dot(rbuf[angle], w, preferred_element_type=jnp.float32)
            sums.append(result[:rows] + result[rows:2 * rows] + result[2 * rows:])
        return jnp.concatenate(sums, axis=1)

    loaded = angles * cb * out.shape[1] // (rows * pairs * LANES)
    settled(loaded + 6 * regions - 5, loaded + 4 * regions - 4, 0)
    out[...] = projected(range(regions - 1))
    settled(3, 2, 1)
    out[...] += projected([regions - 1])


def body(projections, flats, block_start, bp_weights):
    _, rows, width = projections.shape
    angles, cb, pixels = bp_weights.shape
    regions, tiles = lax.axis_size("ang"), lax.axis_size("row")
    cs = LANES // (2 * rows)
    pairs = cb // cs // 2
    table = jnp.asarray(filter_table(rows + 2 * HALO, width, cs), jnp.bfloat16)
    hbm = pl.BlockSpec(memory_space=pltpu.HBM)
    return pl.pallas_call(
        functools.partial(kernel, regions, tiles),
        name="fbp",
        out_shape=pltpu.VMEM((rows, pixels), jnp.float32),
        in_specs=[hbm, hbm, hbm, hbm, hbm],
        out_specs=pl.BlockSpec(memory_space=pltpu.VMEM),
        scratch_shapes=[
            pltpu.SMEM(block_start.shape, jnp.int32),
            pltpu.VMEM((rows, width), jnp.bfloat16),
            pltpu.VMEM((rows, width), jnp.float32),
            pltpu.VMEM(table.shape, jnp.bfloat16),
            pltpu.VMEM(bp_weights.shape, jnp.bfloat16),
            pltpu.VMEM((2 * width // LANES, rows, LANES), jnp.float32),
            pltpu.VMEM((regions * (cb // cs) * rows, width), jnp.bfloat16),
            pltpu.VMEM((6 * regions + bp_weights.size // (rows * pairs * LANES), rows, pairs * LANES), jnp.bfloat16),
            pltpu.VMEM((angles, 3 * rows, pairs * LANES), jnp.bfloat16),
            pltpu.SemaphoreType.DMA((4,)),
            pltpu.SemaphoreType.DMA((2,)),
        ],
        compiler_params=pltpu.CompilerParams(collective_id=0, has_side_effects=True, vmem_limit_bytes=65000000),
    )(block_start, projections, flats, table, bp_weights)


def solution(mesh):
    placed = (P(("scan", "ang"), "row", None), P(("scan", "row"), None), P(), P(None, None, "ang"))
    return jax.shard_map(
        body, mesh=mesh, in_specs=placed, out_specs=P(("scan", "row"), "ang"), check_vma=False
    )
```

```python
import functools

import jax
import jax.numpy as jnp
import numpy as np
from jax import lax
from jax.experimental import pallas as pl
from jax.experimental.pallas import tpu as pltpu
from jax.sharding import PartitionSpec as P

HALO = 4
LANES = 128
FLAT_CUTS = 2
TABLE_CUTS = 2
CENTRE = 4
EARLY = 4
paganin_beta = 8.0
ramp_gain = 320.0


def filter_table(tile_rows, width, columns):
    u = np.arange(tile_rows, dtype=np.float64)
    v = np.arange(width, dtype=np.float64)
    lam = (4.0 * np.sin(np.pi * u / tile_rows) ** 2)[:, None] + (4.0 * np.sin(np.pi * v / width) ** 2)[None, :]
    folded = np.minimum(v, width - v)
    ramp = ramp_gain * (folded / width) * (0.5 + 0.5 * np.cos(2.0 * np.pi * folded / width))
    taps = np.real(np.fft.ifft2(ramp[None, :] / (1.0 + paganin_beta * lam)))
    lags = tile_rows // 2 + 1
    place = (np.arange(columns)[:, None] - np.arange(width)[None, :]) % width
    sign = np.where(np.arange(width) < width // LANES // 2 * LANES, 1.0, -1.0)
    return taps[:lags][:, place].reshape(lags * columns, width) * sign


def kernel(regions, tiles, starts, proj, flats, table, weights, out,
           starts_s, proj_v, flats_v, table_v, weights_v, xs, ys, sbuf, rbuf,
           load_sem, done_sem):
    rows, width = flats.shape
    blocks = width // LANES
    angles, cb, _ = weights.shape
    half = rows // 2
    cs = LANES // (2 * rows)
    shifts = cb // cs
    pairs = shifts // 2
    lags = rows + 1
    order = [(0, 0), (1, 0), *[(0, d) for d in range(1, rows)], (1, rows - 1), *[(1, d) for d in range(1, rows - 1)]]
    me = lax.axis_index("ang")
    row = lax.axis_index("row")

    def peer(step, delta):
        return {"ang": lax.rem(me + step, regions), "row": lax.rem(row + delta + tiles, tiles)}

    def when_there(delta, action):
        if delta == 0:
            action()
        else:
            pl.when(row > 0 if delta < 0 else row < tiles - 1)(action)

    start_load = pltpu.make_async_copy(starts, starts_s, load_sem.at[2])
    table_load = pltpu.make_async_copy(table, table_v, load_sem.at[3])
    weight_load = pltpu.make_async_copy(weights, weights_v, done_sem.at[0])

    def load_columns(begin, end, cuts, sem):
        for n in range(cuts):
            part = pl.ds((begin + n * (end - begin) // cuts) * LANES, (end - begin) // cuts * LANES)
            pltpu.make_async_copy(flats.at[:, part], flats_v.at[:, part], sem).start()
        part = pl.ds(begin * LANES, (end - begin) * LANES)
        pltpu.make_async_copy(proj.at[0, :, part], proj_v.at[:, part], sem).start()

    def columns_loaded(count, sem):
        both = xs.at[pl.ds(0, count * 3 // 2)]
        pltpu.make_async_copy(both, both, sem).wait()

    load_columns(0, CENTRE, 1, load_sem.at[0])
    load_columns(CENTRE, blocks, FLAT_CUTS, load_sem.at[1])
    start_load.start()
    for d in range(lags):
        for n in range(TABLE_CUTS):
            part = pl.ds(n * width // TABLE_CUTS, width // TABLE_CUTS)
            pltpu.make_async_copy(table.at[pl.ds(d * cs, cs), part], table_v.at[pl.ds(d * cs, cs), part], load_sem.at[3]).start()
    weight_load.start()

    barrier = pltpu.get_barrier_semaphore()
    def greet(delta):
        for step in range(regions):
            if (step, delta) != (0, 0):
                pl.semaphore_signal(barrier, inc=1, device_id=peer(step, delta), device_id_type=pl.DeviceIdType.MESH)

    for delta in (-1, 0, 1):
        when_there(delta, lambda: greet(delta))

    def slot(delta):
        return pl.ds((1 + delta) * rows, rows)

    zeros = jnp.zeros((angles, rows, pairs * LANES), jnp.bfloat16)
    pl.when(row == tiles - 1)(lambda: rbuf.at[:, slot(-1)].__setitem__(..., zeros))
    pl.when(row == 0)(lambda: rbuf.at[:, slot(1)].__setitem__(..., zeros))

    lane = lax.broadcasted_iota(jnp.int32, (rows, LANES), 1)
    sub = lax.broadcasted_iota(jnp.int32, (rows, LANES), 0)

    pieces = [slice(b * LANES, (b + 1) * LANES) for b in range(blocks)]

    def contrast_of(p):
        return 1.0 - proj_v[:, p].astype(jnp.float32) / flats_v[:, p]

    columns_loaded(CENTRE, load_sem.at[0])
    contrast = [contrast_of(p) for p in pieces[:CENTRE]]
    centre = jnp.sum(sum(contrast), axis=1, keepdims=True) / (CENTRE * LANES)
    columns_loaded(blocks - CENTRE, load_sem.at[1])
    start_load.wait()

    contrast += [contrast_of(p) for p in pieces[CENTRE:]]
    for b, x in enumerate(contrast):
        xs[b] = x - centre
        xs[b + blocks] = x - centre

    spot = lane // cs
    lag = jnp.where(spot < 2, 0, jnp.where(spot < rows, spot - 1, jnp.where(spot < rows + 2, rows - 1, spot - rows - 1)))
    odd = (spot == 1) | (spot > rows)
    up, down = lax.rem(sub + rows - lag, rows), lax.rem(sub + lag, rows)
    inside = [sub >= lag, (lag > 0) & (sub + lag < rows)]
    wrapped = [(sub < lag) | (lag == 0), sub + lag >= rows]
    parts = {-1: [wrapped[0] & (up < half), wrapped[1] & (down < half)],
             1: [wrapped[0] & (up >= half), wrapped[1] & (down >= half)],
             0: inside}
    bits = [1 << n for n in range((rows - 1).bit_length())]
    deep = shifts * rows

    def shifted_rows(group, members=range(blocks)):
        used = sorted({b + n for b in members for n in (0, 1)})
        for region in group:
            shifted = []
            for k in range(shifts):
                start = starts_s[me, region] + k * cs
                first = start // LANES
                rest = lax.rem(start, LANES)
                shift = lax.rem(LANES - rest, LANES)
                low = lane < LANES - rest
                turned = {b: pltpu.roll(xs[first + b], shift, 1) for b in used}
                shifted.append({b: jnp.where(low, turned[b], turned[b + 1]) for b in members})
            for b in members:
                place = region * deep
                ys[place:place + deep, pieces[b]] = jnp.concatenate(
                    [y[b] for y in shifted], axis=0).astype(jnp.bfloat16)

    def filtered(group):
        cut = blocks // 2 * LANES
        begin = group[0] * deep
        end = begin + len(group) * deep
        near, far = (lax.dot_general(
            ys[begin:end, part], jnp.concatenate([table_v[d * cs:(d + 1) * cs, part] for _, d in [*order, (0, rows), (1, rows)]], axis=0),
            (((1,), (1,)), ((), ())), preferred_element_type=jnp.float32) for part in (slice(cut), slice(cut, width)))
        total = near - far
        total = jnp.concatenate([total, jnp.zeros((total.shape[0], LANES - 2 * cs), jnp.float32)], axis=1)
        for n, region in enumerate(group):
            for k in range(pairs):
                base = n * deep + k * 2 * rows
                even_rows, odd_rows = total[base:base + rows], total[base + rows:base + 2 * rows]
                tile = jnp.where(odd, odd_rows[:, :LANES], even_rows[:, :LANES])
                last = jnp.where(odd, odd_rows[:, LANES:], even_rows[:, LANES:])
                ahead, back = tile, tile
                for bit in bits:
                    turn = (lag & bit) > 0
                    ahead = jnp.where(turn, pltpu.roll(ahead, bit, 0), ahead)
                    back = jnp.where(turn, pltpu.roll(back, rows - bit, 0), back)
                edge = jnp.where(lag == 0, last, ahead)
                for delta, (first, second) in parts.items():
                    value = jnp.where(first, edge if delta else ahead, 0.0) + jnp.where(second, back, 0.0)
                    sbuf[(1 + delta) * regions + region, :, k * LANES:(k + 1) * LANES] = value.astype(jnp.bfloat16)

    def send(group):
        for region in group:
            last = (region + (regions - 1 if region < regions // 2 else 1)) % regions
            final = (me == last).astype(jnp.int32)
            for delta in (-1, 1, 0):
                copy = pltpu.make_async_remote_copy(
                    src_ref=sbuf.at[(1 + delta) * regions + region], dst_ref=rbuf.at[me, slot(delta)],
                    send_sem=done_sem.at[0], recv_sem=done_sem.at[final],
                    device_id={"ang": region, "row": lax.rem(row + delta + tiles, tiles)},
                    device_id_type=pl.DeviceIdType.MESH)
                if delta == 0:
                    pl.when(me != region)(copy.start)
                else:
                    when_there(delta, copy.start)

    early = [b for b in range(blocks) if b % (blocks // 2) < EARLY]
    shifted_rows([0], early)
    table_load.wait()
    shifted_rows([0], [b for b in range(blocks) if b not in early])
    filtered([0])
    sides = (row > 0).astype(jnp.int32) + (row < tiles - 1).astype(jnp.int32)
    pl.semaphore_wait(barrier, regions - 1 + sides * regions)
    send([0])
    shifted_rows([*range(1, regions)])
    filtered([*range(1, regions)])
    send([*range(1, regions)])
    rbuf[me, slot(0)] = sbuf[regions + me]

    inner = (row > 0) & (row < tiles - 1)
    turn = jnp.where(me < regions // 2, 1, regions - 1)

    def source(step):
        return lax.rem(me + step * turn, regions)

    def settled(full, short, sem):
        def wait(count):
            units = sbuf.at[pl.ds(0, count)]
            pltpu.make_async_copy(units, units, done_sem.at[sem]).wait()

        pl.when(inner)(lambda: wait(full))
        pl.when(jnp.logical_not(inner))(lambda: wait(short))

    def projected(steps):
        sums = []
        for half_pixels in range(2):
            pixels = pl.ds(half_pixels * (out.shape[1] // 2), out.shape[1] // 2)
            result = 0.0
            for step in steps:
                angle = source(step)
                w = jnp.concatenate(
                    [weights_v[angle, (2 * k + side) * cs:(2 * k + side + 1) * cs, pixels]
                     for k in range(pairs) for side, _ in order], axis=0)
                result += jnp.dot(rbuf[angle], w, preferred_element_type=jnp.float32)
            sums.append(result[:rows] + result[rows:2 * rows] + result[2 * rows:])
        return jnp.concatenate(sums, axis=1)

    loaded = angles * cb * out.shape[1] // (rows * pairs * LANES)
    settled(loaded + 6 * regions - 5, loaded + 4 * regions - 4, 0)
    out[...] = projected(range(regions - 1))
    settled(3, 2, 1)
    out[...] += projected([regions - 1])


def body(projections, flats, block_start, bp_weights):
    _, rows, width = projections.shape
    angles, cb, pixels = bp_weights.shape
    regions, tiles = lax.axis_size("ang"), lax.axis_size("row")
    cs = LANES // (2 * rows)
    pairs = cb // cs // 2
    table = jnp.asarray(filter_table(rows + 2 * HALO, width, cs), jnp.bfloat16)
    hbm = pl.BlockSpec(memory_space=pltpu.HBM)
    return pl.pallas_call(
        functools.partial(kernel, regions, tiles),
        name="fbp",
        out_shape=pltpu.VMEM((rows, pixels), jnp.float32),
        in_specs=[hbm, hbm, hbm, hbm, hbm],
        out_specs=pl.BlockSpec(memory_space=pltpu.VMEM),
        scratch_shapes=[
            pltpu.SMEM(block_start.shape, jnp.int32),
            pltpu.VMEM((rows, width), jnp.bfloat16),
            pltpu.VMEM((rows, width), jnp.float32),
            pltpu.VMEM(table.shape, jnp.bfloat16),
            pltpu.VMEM(bp_weights.shape, jnp.bfloat16),
            pltpu.VMEM((2 * width // LANES, rows, LANES), jnp.float32),
            pltpu.VMEM((regions * (cb // cs) * rows, width), jnp.bfloat16),
            pltpu.VMEM((6 * regions + bp_weights.size // (rows * pairs * LANES), rows, pairs * LANES), jnp.bfloat16),
            pltpu.VMEM((angles, 3 * rows, pairs * LANES), jnp.bfloat16),
            pltpu.SemaphoreType.DMA((4,)),
            pltpu.SemaphoreType.DMA((2,)),
        ],
        compiler_params=pltpu.CompilerParams(collective_id=0, has_side_effects=True, vmem_limit_bytes=65000000),
    )(block_start, projections, flats, table, bp_weights)


def solution(mesh):
    placed = (P(("scan", "ang"), "row", None), P(("scan", "row"), None), P(), P(None, None, "ang"))
    return jax.shard_map(
        body, mesh=mesh, in_specs=placed, out_specs=P(("scan", "row"), "ang"), check_vma=False
    )
```

```python
import functools

import jax
import jax.numpy as jnp
import numpy as np
from jax import lax
from jax.experimental import pallas as pl
from jax.experimental.pallas import tpu as pltpu
from jax.sharding import PartitionSpec as P

HALO = 4
LANES = 128
FLAT_CUTS = 2
TABLE_CUTS = 2
CENTRE = 10
EARLY = 4
paganin_beta = 8.0
ramp_gain = 320.0


def filter_table(tile_rows, width, columns):
    u = np.arange(tile_rows, dtype=np.float64)
    v = np.arange(width, dtype=np.float64)
    lam = (4.0 * np.sin(np.pi * u / tile_rows) ** 2)[:, None] + (4.0 * np.sin(np.pi * v / width) ** 2)[None, :]
    folded = np.minimum(v, width - v)
    ramp = ramp_gain * (folded / width) * (0.5 + 0.5 * np.cos(2.0 * np.pi * folded / width))
    taps = np.real(np.fft.ifft2(ramp[None, :] / (1.0 + paganin_beta * lam)))
    lags = tile_rows // 2 + 1
    place = (np.arange(columns)[:, None] - np.arange(width)[None, :]) % width
    sign = np.where(np.arange(width) < width // LANES // 2 * LANES, 1.0, -1.0)
    return taps[:lags][:, place].reshape(lags * columns, width) * sign


def kernel(regions, tiles, starts, proj, flats, table, weights, out,
           starts_s, proj_v, flats_v, table_v, weights_v, xs, ys, sbuf, rbuf,
           load_sem, done_sem):
    rows, width = flats.shape
    blocks = width // LANES
    angles, cb, _ = weights.shape
    half = rows // 2
    cs = LANES // (2 * rows)
    shifts = cb // cs
    pairs = shifts // 2
    lags = rows + 1
    order = [(0, 0), (1, 0), *[(0, d) for d in range(1, rows)], (1, rows - 1), *[(1, d) for d in range(1, rows - 1)]]
    me = lax.axis_index("ang")
    row = lax.axis_index("row")

    def peer(step, delta):
        return {"ang": lax.rem(me + step, regions), "row": lax.rem(row + delta + tiles, tiles)}

    def when_there(delta, action):
        if delta == 0:
            action()
        else:
            pl.when(row > 0 if delta < 0 else row < tiles - 1)(action)

    start_load = pltpu.make_async_copy(starts, starts_s, load_sem.at[2])
    table_load = pltpu.make_async_copy(table, table_v, load_sem.at[3])
    weight_load = pltpu.make_async_copy(weights, weights_v, done_sem.at[0])

    def load_columns(begin, end, cuts, sem):
        for n in range(cuts):
            part = pl.ds((begin + n * (end - begin) // cuts) * LANES, (end - begin) // cuts * LANES)
            pltpu.make_async_copy(flats.at[:, part], flats_v.at[:, part], sem).start()
        part = pl.ds(begin * LANES, (end - begin) * LANES)
        pltpu.make_async_copy(proj.at[0, :, part], proj_v.at[:, part], sem).start()

    def columns_loaded(count, sem):
        both = xs.at[pl.ds(0, count * 3 // 2)]
        pltpu.make_async_copy(both, both, sem).wait()

    load_columns(0, CENTRE, 1, load_sem.at[0])
    load_columns(CENTRE, blocks, FLAT_CUTS, load_sem.at[1])
    start_load.start()
    for d in range(lags):
        for n in range(TABLE_CUTS):
            part = pl.ds(n * width // TABLE_CUTS, width // TABLE_CUTS)
            pltpu.make_async_copy(table.at[pl.ds(d * cs, cs), part], table_v.at[pl.ds(d * cs, cs), part], load_sem.at[3]).start()
    weight_load.start()

    barrier = pltpu.get_barrier_semaphore()
    def greet(delta):
        for step in range(regions):
            if (step, delta) != (0, 0):
                pl.semaphore_signal(barrier, inc=1, device_id=peer(step, delta), device_id_type=pl.DeviceIdType.MESH)

    for delta in (-1, 0, 1):
        when_there(delta, lambda: greet(delta))

    def slot(delta):
        return pl.ds((1 + delta) * rows, rows)

    zeros = jnp.zeros((angles, rows, pairs * LANES), jnp.bfloat16)
    pl.when(row == tiles - 1)(lambda: rbuf.at[:, slot(-1)].__setitem__(..., zeros))
    pl.when(row == 0)(lambda: rbuf.at[:, slot(1)].__setitem__(..., zeros))

    lane = lax.broadcasted_iota(jnp.int32, (rows, LANES), 1)
    sub = lax.broadcasted_iota(jnp.int32, (rows, LANES), 0)

    pieces = [slice(b * LANES, (b + 1) * LANES) for b in range(blocks)]

    def contrast_of(p):
        return 1.0 - proj_v[:, p].astype(jnp.float32) / flats_v[:, p]

    columns_loaded(CENTRE, load_sem.at[0])
    contrast = [contrast_of(p) for p in pieces[:CENTRE]]
    centre = jnp.sum(sum(contrast), axis=1, keepdims=True) / (CENTRE * LANES)
    columns_loaded(blocks - CENTRE, load_sem.at[1])
    start_load.wait()

    contrast += [contrast_of(p) for p in pieces[CENTRE:]]
    for b, x in enumerate(contrast):
        xs[b] = x - centre
        xs[b + blocks] = x - centre

    spot = lane // cs
    lag = jnp.where(spot < 2, 0, jnp.where(spot < rows, spot - 1, jnp.where(spot < rows + 2, rows - 1, spot - rows - 1)))
    odd = (spot == 1) | (spot > rows)
    up, down = lax.rem(sub + rows - lag, rows), lax.rem(sub + lag, rows)
    inside = [sub >= lag, (lag > 0) & (sub + lag < rows)]
    wrapped = [(sub < lag) | (lag == 0), sub + lag >= rows]
    parts = {-1: [wrapped[0] & (up < half), wrapped[1] & (down < half)],
             1: [wrapped[0] & (up >= half), wrapped[1] & (down >= half)],
             0: inside}
    bits = [1 << n for n in range((rows - 1).bit_length())]
    deep = shifts * rows

    def shifted_rows(group, members=range(blocks)):
        used = sorted({b + n for b in members for n in (0, 1)})
        for region in group:
            shifted = []
            for k in range(shifts):
                start = starts_s[me, region] + k * cs
                first = start // LANES
                rest = lax.rem(start, LANES)
                shift = lax.rem(LANES - rest, LANES)
                low = lane < LANES - rest
                turned = {b: pltpu.roll(xs[first + b], shift, 1) for b in used}
                shifted.append({b: jnp.where(low, turned[b], turned[b + 1]) for b in members})
            for b in members:
                place = region * deep
                ys[place:place + deep, pieces[b]] = jnp.concatenate(
                    [y[b] for y in shifted], axis=0).astype(jnp.bfloat16)

    def filtered(group):
        cut = blocks // 2 * LANES
        begin = group[0] * deep
        end = begin + len(group) * deep
        near, far = (lax.dot_general(
            ys[begin:end, part], jnp.concatenate([table_v[d * cs:(d + 1) * cs, part] for _, d in [*order, (0, rows), (1, rows)]], axis=0),
            (((1,), (1,)), ((), ())), preferred_element_type=jnp.float32) for part in (slice(cut), slice(cut, width)))
        total = near - far
        total = jnp.concatenate([total, jnp.zeros((total.shape[0], LANES - 2 * cs), jnp.float32)], axis=1)
        for n, region in enumerate(group):
            for k in range(pairs):
                base = n * deep + k * 2 * rows
                even_rows, odd_rows = total[base:base + rows], total[base + rows:base + 2 * rows]
                tile = jnp.where(odd, odd_rows[:, :LANES], even_rows[:, :LANES])
                last = jnp.where(odd, odd_rows[:, LANES:], even_rows[:, LANES:])
                ahead, back = tile, tile
                for bit in bits:
                    turn = (lag & bit) > 0
                    ahead = jnp.where(turn, pltpu.roll(ahead, bit, 0), ahead)
                    back = jnp.where(turn, pltpu.roll(back, rows - bit, 0), back)
                edge = jnp.where(lag == 0, last, ahead)
                for delta, (first, second) in parts.items():
                    value = jnp.where(first, edge if delta else ahead, 0.0) + jnp.where(second, back, 0.0)
                    sbuf[(1 + delta) * regions + region, :, k * LANES:(k + 1) * LANES] = value.astype(jnp.bfloat16)

    def send(group):
        for region in group:
            last = (region + (regions - 1 if region < regions // 2 else 1)) % regions
            final = (me == last).astype(jnp.int32)
            for delta in (-1, 1, 0):
                copy = pltpu.make_async_remote_copy(
                    src_ref=sbuf.at[(1 + delta) * regions + region], dst_ref=rbuf.at[me, slot(delta)],
                    send_sem=done_sem.at[0], recv_sem=done_sem.at[final],
                    device_id={"ang": region, "row": lax.rem(row + delta + tiles, tiles)},
                    device_id_type=pl.DeviceIdType.MESH)
                if delta == 0:
                    pl.when(me != region)(copy.start)
                else:
                    when_there(delta, copy.start)

    early = [b for b in range(blocks) if b % (blocks // 2) < EARLY]
    shifted_rows([0], early)
    table_load.wait()
    shifted_rows([0], [b for b in range(blocks) if b not in early])
    filtered([0])
    sides = (row > 0).astype(jnp.int32) + (row < tiles - 1).astype(jnp.int32)
    pl.semaphore_wait(barrier, regions - 1 + sides * regions)
    send([0])
    shifted_rows([*range(1, regions)])
    filtered([*range(1, regions)])
    send([*range(1, regions)])
    rbuf[me, slot(0)] = sbuf[regions + me]

    inner = (row > 0) & (row < tiles - 1)
    turn = jnp.where(me < regions // 2, 1, regions - 1)

    def source(step):
        return lax.rem(me + step * turn, regions)

    def settled(full, short, sem):
        def wait(count):
            units = sbuf.at[pl.ds(0, count)]
            pltpu.make_async_copy(units, units, done_sem.at[sem]).wait()

        pl.when(inner)(lambda: wait(full))
        pl.when(jnp.logical_not(inner))(lambda: wait(short))

    def projected(steps):
        sums = []
        for half_pixels in range(2):
            pixels = pl.ds(half_pixels * (out.shape[1] // 2), out.shape[1] // 2)
            result = 0.0
            for step in steps:
                angle = source(step)
                w = jnp.concatenate(
                    [weights_v[angle, (2 * k + side) * cs:(2 * k + side + 1) * cs, pixels]
                     for k in range(pairs) for side, _ in order], axis=0)
                result += jnp.dot(rbuf[angle], w, preferred_element_type=jnp.float32)
            sums.append(result[:rows] + result[rows:2 * rows] + result[2 * rows:])
        return jnp.concatenate(sums, axis=1)

    loaded = angles * cb * out.shape[1] // (rows * pairs * LANES)
    settled(loaded + 6 * regions - 5, loaded + 4 * regions - 4, 0)
    out[...] = projected(range(regions - 1))
    settled(3, 2, 1)
    out[...] += projected([regions - 1])


def body(projections, flats, block_start, bp_weights):
    _, rows, width = projections.shape
    angles, cb, pixels = bp_weights.shape
    regions, tiles = lax.axis_size("ang"), lax.axis_size("row")
    cs = LANES // (2 * rows)
    pairs = cb // cs // 2
    table = jnp.asarray(filter_table(rows + 2 * HALO, width, cs), jnp.bfloat16)
    hbm = pl.BlockSpec(memory_space=pltpu.HBM)
    return pl.pallas_call(
        functools.partial(kernel, regions, tiles),
        name="fbp",
        out_shape=pltpu.VMEM((rows, pixels), jnp.float32),
        in_specs=[hbm, hbm, hbm, hbm, hbm],
        out_specs=pl.BlockSpec(memory_space=pltpu.VMEM),
        scratch_shapes=[
            pltpu.SMEM(block_start.shape, jnp.int32),
            pltpu.VMEM((rows, width), jnp.bfloat16),
            pltpu.VMEM((rows, width), jnp.float32),
            pltpu.VMEM(table.shape, jnp.bfloat16),
            pltpu.VMEM(bp_weights.shape, jnp.bfloat16),
            pltpu.VMEM((2 * width // LANES, rows, LANES), jnp.float32),
            pltpu.VMEM((regions * (cb // cs) * rows, width), jnp.bfloat16),
            pltpu.VMEM((6 * regions + bp_weights.size // (rows * pairs * LANES), rows, pairs * LANES), jnp.bfloat16),
            pltpu.VMEM((angles, 3 * rows, pairs * LANES), jnp.bfloat16),
            pltpu.SemaphoreType.DMA((4,)),
            pltpu.SemaphoreType.DMA((2,)),
        ],
        compiler_params=pltpu.CompilerParams(collective_id=0, has_side_effects=True, vmem_limit_bytes=65000000),
    )(block_start, projections, flats, table, bp_weights)


def solution(mesh):
    placed = (P(("scan", "ang"), "row", None), P(("scan", "row"), None), P(), P(None, None, "ang"))
    return jax.shard_map(
        body, mesh=mesh, in_specs=placed, out_specs=P(("scan", "row"), "ang"), check_vma=False
    )
```

```python
import functools

import jax
import jax.numpy as jnp
import numpy as np
from jax import lax
from jax.experimental import pallas as pl
from jax.experimental.pallas import tpu as pltpu
from jax.sharding import PartitionSpec as P

HALO = 4
LANES = 128
FLAT_CUTS = 2
TABLE_CUTS = 2
CENTRE = 4
EARLY = 4
paganin_beta = 8.0
ramp_gain = 320.0


def filter_table(tile_rows, width, columns):
    u = np.arange(tile_rows, dtype=np.float64)
    v = np.arange(width, dtype=np.float64)
    lam = (4.0 * np.sin(np.pi * u / tile_rows) ** 2)[:, None] + (4.0 * np.sin(np.pi * v / width) ** 2)[None, :]
    folded = np.minimum(v, width - v)
    ramp = ramp_gain * (folded / width) * (0.5 + 0.5 * np.cos(2.0 * np.pi * folded / width))
    taps = np.real(np.fft.ifft2(ramp[None, :] / (1.0 + paganin_beta * lam)))
    lags = tile_rows // 2 + 1
    place = (np.arange(columns)[:, None] - np.arange(width)[None, :]) % width
    sign = np.where(np.arange(width) < width // LANES // 2 * LANES, 1.0, -1.0)
    return taps[:lags][:, place].reshape(lags * columns, width) * sign


def kernel(regions, tiles, starts, proj, flats, table, weights, out,
           starts_s, proj_v, flats_v, table_v, weights_v, xs, ys, sbuf, rbuf,
           load_sem, done_sem):
    rows, width = flats.shape
    blocks = width // LANES
    angles, cb, _ = weights.shape
    half = rows // 2
    cs = LANES // (2 * rows)
    shifts = cb // cs
    pairs = shifts // 2
    lags = rows + 1
    order = [(0, 0), (1, 0), *[(0, d) for d in range(1, rows)], (1, rows - 1), *[(1, d) for d in range(1, rows - 1)]]
    me = lax.axis_index("ang")
    row = lax.axis_index("row")

    def peer(step, delta):
        return {"ang": lax.rem(me + step, regions), "row": lax.rem(row + delta + tiles, tiles)}

    def when_there(delta, action):
        if delta == 0:
            action()
        else:
            pl.when(row > 0 if delta < 0 else row < tiles - 1)(action)

    start_load = pltpu.make_async_copy(starts, starts_s, load_sem.at[1])
    table_load = pltpu.make_async_copy(table, table_v, load_sem.at[2])
    weight_load = pltpu.make_async_copy(weights, weights_v, done_sem.at[0])

    def load_columns(begin, end, cuts, sem):
        for n in range(cuts):
            part = pl.ds((begin + n * (end - begin) // cuts) * LANES, (end - begin) // cuts * LANES)
            pltpu.make_async_copy(flats.at[:, part], flats_v.at[:, part], sem).start()
        part = pl.ds(begin * LANES, (end - begin) * LANES)
        pltpu.make_async_copy(proj.at[0, :, part], proj_v.at[:, part], sem).start()

    def columns_loaded(count, sem):
        both = xs.at[pl.ds(0, count * 3 // 2)]
        pltpu.make_async_copy(both, both, sem).wait()

    load_columns(0, blocks, FLAT_CUTS, load_sem.at[0])
    start_load.start()
    for d in range(lags):
        for n in range(TABLE_CUTS):
            part = pl.ds(n * width // TABLE_CUTS, width // TABLE_CUTS)
            pltpu.make_async_copy(table.at[pl.ds(d * cs, cs), part], table_v.at[pl.ds(d * cs, cs), part], load_sem.at[2]).start()
    weight_load.start()

    barrier = pltpu.get_barrier_semaphore()
    def greet(delta):
        for step in range(regions):
            if (step, delta) != (0, 0):
                pl.semaphore_signal(barrier, inc=1, device_id=peer(step, delta), device_id_type=pl.DeviceIdType.MESH)

    for delta in (-1, 0, 1):
        when_there(delta, lambda: greet(delta))

    def slot(delta):
        return pl.ds((1 + delta) * rows, rows)

    zeros = jnp.zeros((angles, rows, pairs * LANES), jnp.bfloat16)
    pl.when(row == tiles - 1)(lambda: rbuf.at[:, slot(-1)].__setitem__(..., zeros))
    pl.when(row == 0)(lambda: rbuf.at[:, slot(1)].__setitem__(..., zeros))

    lane = lax.broadcasted_iota(jnp.int32, (rows, LANES), 1)
    sub = lax.broadcasted_iota(jnp.int32, (rows, LANES), 0)

    pieces = [slice(b * LANES, (b + 1) * LANES) for b in range(blocks)]

    def contrast_of(p):
        return 1.0 - proj_v[:, p].astype(jnp.float32) / flats_v[:, p]

    columns_loaded(blocks, load_sem.at[0])
    start_load.wait()

    contrast = [contrast_of(p) for p in pieces]
    centre = jnp.sum(sum(contrast[:CENTRE]), axis=1, keepdims=True) / (CENTRE * LANES)
    for b, x in enumerate(contrast):
        xs[b] = x - centre
        xs[b + blocks] = x - centre

    spot = lane // cs
    lag = jnp.where(spot < 2, 0, jnp.where(spot < rows, spot - 1, jnp.where(spot < rows + 2, rows - 1, spot - rows - 1)))
    odd = (spot == 1) | (spot > rows)
    up, down = lax.rem(sub + rows - lag, rows), lax.rem(sub + lag, rows)
    inside = [sub >= lag, (lag > 0) & (sub + lag < rows)]
    wrapped = [(sub < lag) | (lag == 0), sub + lag >= rows]
    parts = {-1: [wrapped[0] & (up < half), wrapped[1] & (down < half)],
             1: [wrapped[0] & (up >= half), wrapped[1] & (down >= half)],
             0: inside}
    bits = [1 << n for n in range((rows - 1).bit_length())]
    deep = shifts * rows

    def shifted_rows(group, members=range(blocks)):
        used = sorted({b + n for b in members for n in (0, 1)})
        for region in group:
            shifted = []
            for k in range(shifts):
                start = starts_s[me, region] + k * cs
                first = start // LANES
                rest = lax.rem(start, LANES)
                shift = lax.rem(LANES - rest, LANES)
                low = lane < LANES - rest
                turned = {b: pltpu.roll(xs[first + b], shift, 1) for b in used}
                shifted.append({b: jnp.where(low, turned[b], turned[b + 1]) for b in members})
            for b in members:
                place = region * deep
                ys[place:place + deep, pieces[b]] = jnp.concatenate(
                    [y[b] for y in shifted], axis=0).astype(jnp.bfloat16)

    def filtered(group):
        cut = blocks // 2 * LANES
        begin = group[0] * deep
        end = begin + len(group) * deep
        near, far = (lax.dot_general(
            ys[begin:end, part], jnp.concatenate([table_v[d * cs:(d + 1) * cs, part] for _, d in [*order, (0, rows), (1, rows)]], axis=0),
            (((1,), (1,)), ((), ())), preferred_element_type=jnp.float32) for part in (slice(cut), slice(cut, width)))
        total = near - far
        total = jnp.concatenate([total, jnp.zeros((total.shape[0], LANES - 2 * cs), jnp.float32)], axis=1)
        for n, region in enumerate(group):
            for k in range(pairs):
                base = n * deep + k * 2 * rows
                even_rows, odd_rows = total[base:base + rows], total[base + rows:base + 2 * rows]
                tile = jnp.where(odd, odd_rows[:, :LANES], even_rows[:, :LANES])
                last = jnp.where(odd, odd_rows[:, LANES:], even_rows[:, LANES:])
                ahead, back = tile, tile
                for bit in bits:
                    turn = (lag & bit) > 0
                    ahead = jnp.where(turn, pltpu.roll(ahead, bit, 0), ahead)
                    back = jnp.where(turn, pltpu.roll(back, rows - bit, 0), back)
                edge = jnp.where(lag == 0, last, ahead)
                for delta, (first, second) in parts.items():
                    value = jnp.where(first, edge if delta else ahead, 0.0) + jnp.where(second, back, 0.0)
                    sbuf[(1 + delta) * regions + region, :, k * LANES:(k + 1) * LANES] = value.astype(jnp.bfloat16)

    def send(group):
        for region in group:
            last = (region + (regions - 1 if region < regions // 2 else 1)) % regions
            final = (me == last).astype(jnp.int32)
            for delta in (-1, 1, 0):
                copy = pltpu.make_async_remote_copy(
                    src_ref=sbuf.at[(1 + delta) * regions + region], dst_ref=rbuf.at[me, slot(delta)],
                    send_sem=done_sem.at[0], recv_sem=done_sem.at[final],
                    device_id={"ang": region, "row": lax.rem(row + delta + tiles, tiles)},
                    device_id_type=pl.DeviceIdType.MESH)
                if delta == 0:
                    pl.when(me != region)(copy.start)
                else:
                    when_there(delta, copy.start)

    early = [b for b in range(blocks) if b % (blocks // 2) < EARLY]
    shifted_rows([0], early)
    table_load.wait()
    shifted_rows([0], [b for b in range(blocks) if b not in early])
    filtered([0])
    sides = (row > 0).astype(jnp.int32) + (row < tiles - 1).astype(jnp.int32)
    pl.semaphore_wait(barrier, regions - 1 + sides * regions)
    send([0])
    shifted_rows([*range(1, regions)])
    filtered([*range(1, regions)])
    send([*range(1, regions)])
    rbuf[me, slot(0)] = sbuf[regions + me]

    inner = (row > 0) & (row < tiles - 1)
    turn = jnp.where(me < regions // 2, 1, regions - 1)

    def source(step):
        return lax.rem(me + step * turn, regions)

    def settled(full, short, sem):
        def wait(count):
            units = sbuf.at[pl.ds(0, count)]
            pltpu.make_async_copy(units, units, done_sem.at[sem]).wait()

        pl.when(inner)(lambda: wait(full))
        pl.when(jnp.logical_not(inner))(lambda: wait(short))

    def projected(steps):
        sums = []
        for half_pixels in range(2):
            pixels = pl.ds(half_pixels * (out.shape[1] // 2), out.shape[1] // 2)
            result = 0.0
            for step in steps:
                angle = source(step)
                w = jnp.concatenate(
                    [weights_v[angle, (2 * k + side) * cs:(2 * k + side + 1) * cs, pixels]
                     for k in range(pairs) for side, _ in order], axis=0)
                result += jnp.dot(rbuf[angle], w, preferred_element_type=jnp.float32)
            sums.append(result[:rows] + result[rows:2 * rows] + result[2 * rows:])
        return jnp.concatenate(sums, axis=1)

    loaded = angles * cb * out.shape[1] // (rows * pairs * LANES)
    settled(loaded + 6 * regions - 5, loaded + 4 * regions - 4, 0)
    out[...] = projected(range(regions - 1))
    settled(3, 2, 1)
    out[...] += projected([regions - 1])


def body(projections, flats, block_start, bp_weights):
    _, rows, width = projections.shape
    angles, cb, pixels = bp_weights.shape
    regions, tiles = lax.axis_size("ang"), lax.axis_size("row")
    cs = LANES // (2 * rows)
    pairs = cb // cs // 2
    table = jnp.asarray(filter_table(rows + 2 * HALO, width, cs), jnp.bfloat16)
    hbm = pl.BlockSpec(memory_space=pltpu.HBM)
    return pl.pallas_call(
        functools.partial(kernel, regions, tiles),
        name="fbp",
        out_shape=pltpu.VMEM((rows, pixels), jnp.float32),
        in_specs=[hbm, hbm, hbm, hbm, hbm],
        out_specs=pl.BlockSpec(memory_space=pltpu.VMEM),
        scratch_shapes=[
            pltpu.SMEM(block_start.shape, jnp.int32),
            pltpu.VMEM((rows, width), jnp.bfloat16),
            pltpu.VMEM((rows, width), jnp.float32),
            pltpu.VMEM(table.shape, jnp.bfloat16),
            pltpu.VMEM(bp_weights.shape, jnp.bfloat16),
            pltpu.VMEM((2 * width // LANES, rows, LANES), jnp.float32),
            pltpu.VMEM((regions * (cb // cs) * rows, width), jnp.bfloat16),
            pltpu.VMEM((6 * regions + bp_weights.size // (rows * pairs * LANES), rows, pairs * LANES), jnp.bfloat16),
            pltpu.VMEM((angles, 3 * rows, pairs * LANES), jnp.bfloat16),
            pltpu.SemaphoreType.DMA((3,)),
            pltpu.SemaphoreType.DMA((2,)),
        ],
        compiler_params=pltpu.CompilerParams(collective_id=0, has_side_effects=True, vmem_limit_bytes=65000000),
    )(block_start, projections, flats, table, bp_weights)


def solution(mesh):
    placed = (P(("scan", "ang"), "row", None), P(("scan", "row"), None), P(), P(None, None, "ang"))
    return jax.shard_map(
        body, mesh=mesh, in_specs=placed, out_specs=P(("scan", "row"), "ang"), check_vma=False
    )
```

```python
import functools

import jax
import jax.numpy as jnp
import numpy as np
from jax import lax
from jax.experimental import pallas as pl
from jax.experimental.pallas import tpu as pltpu
from jax.sharding import PartitionSpec as P

HALO = 4
LANES = 128
FLAT_CUTS = 2
TABLE_CUTS = 2
CENTRE = 10
EARLY = 6
paganin_beta = 8.0
ramp_gain = 320.0


def filter_table(tile_rows, width, columns):
    u = np.arange(tile_rows, dtype=np.float64)
    v = np.arange(width, dtype=np.float64)
    lam = (4.0 * np.sin(np.pi * u / tile_rows) ** 2)[:, None] + (4.0 * np.sin(np.pi * v / width) ** 2)[None, :]
    folded = np.minimum(v, width - v)
    ramp = ramp_gain * (folded / width) * (0.5 + 0.5 * np.cos(2.0 * np.pi * folded / width))
    taps = np.real(np.fft.ifft2(ramp[None, :] / (1.0 + paganin_beta * lam)))
    lags = tile_rows // 2 + 1
    place = (np.arange(columns)[:, None] - np.arange(width)[None, :]) % width
    sign = np.where(np.arange(width) < width // LANES // 2 * LANES, 1.0, -1.0)
    return taps[:lags][:, place].reshape(lags * columns, width) * sign


def kernel(regions, tiles, starts, proj, flats, table, weights, out,
           starts_s, proj_v, flats_v, table_v, weights_v, xs, ys, sbuf, rbuf,
           load_sem, done_sem):
    rows, width = flats.shape
    blocks = width // LANES
    angles, cb, _ = weights.shape
    half = rows // 2
    cs = LANES // (2 * rows)
    shifts = cb // cs
    pairs = shifts // 2
    lags = rows + 1
    order = [(0, 0), (1, 0), *[(0, d) for d in range(1, rows)], (1, rows - 1), *[(1, d) for d in range(1, rows - 1)]]
    me = lax.axis_index("ang")
    row = lax.axis_index("row")

    def peer(step, delta):
        return {"ang": lax.rem(me + step, regions), "row": lax.rem(row + delta + tiles, tiles)}

    def when_there(delta, action):
        if delta == 0:
            action()
        else:
            pl.when(row > 0 if delta < 0 else row < tiles - 1)(action)

    start_load = pltpu.make_async_copy(starts, starts_s, load_sem.at[2])
    table_load = pltpu.make_async_copy(table, table_v, load_sem.at[3])
    weight_load = pltpu.make_async_copy(weights, weights_v, done_sem.at[0])

    def load_columns(begin, end, cuts, sem):
        for n in range(cuts):
            part = pl.ds((begin + n * (end - begin) // cuts) * LANES, (end - begin) // cuts * LANES)
            pltpu.make_async_copy(flats.at[:, part], flats_v.at[:, part], sem).start()
        part = pl.ds(begin * LANES, (end - begin) * LANES)
        pltpu.make_async_copy(proj.at[0, :, part], proj_v.at[:, part], sem).start()

    def columns_loaded(count, sem):
        both = xs.at[pl.ds(0, count * 3 // 2)]
        pltpu.make_async_copy(both, both, sem).wait()

    load_columns(0, CENTRE, 1, load_sem.at[0])
    load_columns(CENTRE, blocks, FLAT_CUTS, load_sem.at[1])
    start_load.start()
    for d in range(lags):
        for n in range(TABLE_CUTS):
            part = pl.ds(n * width // TABLE_CUTS, width // TABLE_CUTS)
            pltpu.make_async_copy(table.at[pl.ds(d * cs, cs), part], table_v.at[pl.ds(d * cs, cs), part], load_sem.at[3]).start()
    weight_load.start()

    barrier = pltpu.get_barrier_semaphore()
    def greet(delta):
        for step in range(regions):
            if (step, delta) != (0, 0):
                pl.semaphore_signal(barrier, inc=1, device_id=peer(step, delta), device_id_type=pl.DeviceIdType.MESH)

    for delta in (-1, 0, 1):
        when_there(delta, lambda: greet(delta))

    def slot(delta):
        return pl.ds((1 + delta) * rows, rows)

    zeros = jnp.zeros((angles, rows, pairs * LANES), jnp.bfloat16)
    pl.when(row == tiles - 1)(lambda: rbuf.at[:, slot(-1)].__setitem__(..., zeros))
    pl.when(row == 0)(lambda: rbuf.at[:, slot(1)].__setitem__(..., zeros))

    lane = lax.broadcasted_iota(jnp.int32, (rows, LANES), 1)
    sub = lax.broadcasted_iota(jnp.int32, (rows, LANES), 0)

    pieces = [slice(b * LANES, (b + 1) * LANES) for b in range(blocks)]

    def contrast_of(p):
        return 1.0 - proj_v[:, p].astype(jnp.float32) / flats_v[:, p]

    columns_loaded(CENTRE, load_sem.at[0])
    contrast = [contrast_of(p) for p in pieces[:CENTRE]]
    centre = jnp.sum(sum(contrast), axis=1, keepdims=True) / (CENTRE * LANES)
    columns_loaded(blocks - CENTRE, load_sem.at[1])
    start_load.wait()

    contrast += [contrast_of(p) for p in pieces[CENTRE:]]
    for b, x in enumerate(contrast):
        xs[b] = x - centre
        xs[b + blocks] = x - centre

    spot = lane // cs
    lag = jnp.where(spot < 2, 0, jnp.where(spot < rows, spot - 1, jnp.where(spot < rows + 2, rows - 1, spot - rows - 1)))
    odd = (spot == 1) | (spot > rows)
    up, down = lax.rem(sub + rows - lag, rows), lax.rem(sub + lag, rows)
    inside = [sub >= lag, (lag > 0) & (sub + lag < rows)]
    wrapped = [(sub < lag) | (lag == 0), sub + lag >= rows]
    parts = {-1: [wrapped[0] & (up < half), wrapped[1] & (down < half)],
             1: [wrapped[0] & (up >= half), wrapped[1] & (down >= half)],
             0: inside}
    bits = [1 << n for n in range((rows - 1).bit_length())]
    deep = shifts * rows

    def shifted_rows(group, members=range(blocks)):
        used = sorted({b + n for b in members for n in (0, 1)})
        for region in group:
            shifted = []
            for k in range(shifts):
                start = starts_s[me, region] + k * cs
                first = start // LANES
                rest = lax.rem(start, LANES)
                shift = lax.rem(LANES - rest, LANES)
                low = lane < LANES - rest
                turned = {b: pltpu.roll(xs[first + b], shift, 1) for b in used}
                shifted.append({b: jnp.where(low, turned[b], turned[b + 1]) for b in members})
            for b in members:
                place = region * deep
                ys[place:place + deep, pieces[b]] = jnp.concatenate(
                    [y[b] for y in shifted], axis=0).astype(jnp.bfloat16)

    def filtered(group):
        cut = blocks // 2 * LANES
        begin = group[0] * deep
        end = begin + len(group) * deep
        near, far = (lax.dot_general(
            ys[begin:end, part], jnp.concatenate([table_v[d * cs:(d + 1) * cs, part] for _, d in [*order, (0, rows), (1, rows)]], axis=0),
            (((1,), (1,)), ((), ())), preferred_element_type=jnp.float32) for part in (slice(cut), slice(cut, width)))
        total = near - far
        total = jnp.concatenate([total, jnp.zeros((total.shape[0], LANES - 2 * cs), jnp.float32)], axis=1)
        for n, region in enumerate(group):
            for k in range(pairs):
                base = n * deep + k * 2 * rows
                even_rows, odd_rows = total[base:base + rows], total[base + rows:base + 2 * rows]
                tile = jnp.where(odd, odd_rows[:, :LANES], even_rows[:, :LANES])
                last = jnp.where(odd, odd_rows[:, LANES:], even_rows[:, LANES:])
                ahead, back = tile, tile
                for bit in bits:
                    turn = (lag & bit) > 0
                    ahead = jnp.where(turn, pltpu.roll(ahead, bit, 0), ahead)
                    back = jnp.where(turn, pltpu.roll(back, rows - bit, 0), back)
                edge = jnp.where(lag == 0, last, ahead)
                for delta, (first, second) in parts.items():
                    value = jnp.where(first, edge if delta else ahead, 0.0) + jnp.where(second, back, 0.0)
                    sbuf[(1 + delta) * regions + region, :, k * LANES:(k + 1) * LANES] = value.astype(jnp.bfloat16)

    def send(group):
        for region in group:
            last = (region + (regions - 1 if region < regions // 2 else 1)) % regions
            final = (me == last).astype(jnp.int32)
            for delta in (-1, 1, 0):
                copy = pltpu.make_async_remote_copy(
                    src_ref=sbuf.at[(1 + delta) * regions + region], dst_ref=rbuf.at[me, slot(delta)],
                    send_sem=done_sem.at[0], recv_sem=done_sem.at[final],
                    device_id={"ang": region, "row": lax.rem(row + delta + tiles, tiles)},
                    device_id_type=pl.DeviceIdType.MESH)
                if delta == 0:
                    pl.when(me != region)(copy.start)
                else:
                    when_there(delta, copy.start)

    early = [b for b in range(blocks) if b % (blocks // 2) < EARLY]
    shifted_rows([0], early)
    table_load.wait()
    shifted_rows([0], [b for b in range(blocks) if b not in early])
    filtered([0])
    sides = (row > 0).astype(jnp.int32) + (row < tiles - 1).astype(jnp.int32)
    pl.semaphore_wait(barrier, regions - 1 + sides * regions)
    send([0])
    shifted_rows([*range(1, regions)])
    filtered([*range(1, regions)])
    send([*range(1, regions)])
    rbuf[me, slot(0)] = sbuf[regions + me]

    inner = (row > 0) & (row < tiles - 1)
    turn = jnp.where(me < regions // 2, 1, regions - 1)

    def source(step):
        return lax.rem(me + step * turn, regions)

    def settled(full, short, sem):
        def wait(count):
            units = sbuf.at[pl.ds(0, count)]
            pltpu.make_async_copy(units, units, done_sem.at[sem]).wait()

        pl.when(inner)(lambda: wait(full))
        pl.when(jnp.logical_not(inner))(lambda: wait(short))

    def projected(steps):
        sums = []
        for half_pixels in range(2):
            pixels = pl.ds(half_pixels * (out.shape[1] // 2), out.shape[1] // 2)
            result = 0.0
            for step in steps:
                angle = source(step)
                w = jnp.concatenate(
                    [weights_v[angle, (2 * k + side) * cs:(2 * k + side + 1) * cs, pixels]
                     for k in range(pairs) for side, _ in order], axis=0)
                result += jnp.dot(rbuf[angle], w, preferred_element_type=jnp.float32)
            sums.append(result[:rows] + result[rows:2 * rows] + result[2 * rows:])
        return jnp.concatenate(sums, axis=1)

    loaded = angles * cb * out.shape[1] // (rows * pairs * LANES)
    settled(loaded + 6 * regions - 5, loaded + 4 * regions - 4, 0)
    out[...] = projected(range(regions - 1))
    settled(3, 2, 1)
    out[...] += projected([regions - 1])


def body(projections, flats, block_start, bp_weights):
    _, rows, width = projections.shape
    angles, cb, pixels = bp_weights.shape
    regions, tiles = lax.axis_size("ang"), lax.axis_size("row")
    cs = LANES // (2 * rows)
    pairs = cb // cs // 2
    table = jnp.asarray(filter_table(rows + 2 * HALO, width, cs), jnp.bfloat16)
    hbm = pl.BlockSpec(memory_space=pltpu.HBM)
    return pl.pallas_call(
        functools.partial(kernel, regions, tiles),
        name="fbp",
        out_shape=pltpu.VMEM((rows, pixels), jnp.float32),
        in_specs=[hbm, hbm, hbm, hbm, hbm],
        out_specs=pl.BlockSpec(memory_space=pltpu.VMEM),
        scratch_shapes=[
            pltpu.SMEM(block_start.shape, jnp.int32),
            pltpu.VMEM((rows, width), jnp.bfloat16),
            pltpu.VMEM((rows, width), jnp.float32),
            pltpu.VMEM(table.shape, jnp.bfloat16),
            pltpu.VMEM(bp_weights.shape, jnp.bfloat16),
            pltpu.VMEM((2 * width // LANES, rows, LANES), jnp.float32),
            pltpu.VMEM((regions * (cb // cs) * rows, width), jnp.bfloat16),
            pltpu.VMEM((6 * regions + bp_weights.size // (rows * pairs * LANES), rows, pairs * LANES), jnp.bfloat16),
            pltpu.VMEM((angles, 3 * rows, pairs * LANES), jnp.bfloat16),
            pltpu.SemaphoreType.DMA((4,)),
            pltpu.SemaphoreType.DMA((2,)),
        ],
        compiler_params=pltpu.CompilerParams(collective_id=0, has_side_effects=True, vmem_limit_bytes=65000000),
    )(block_start, projections, flats, table, bp_weights)


def solution(mesh):
    placed = (P(("scan", "ang"), "row", None), P(("scan", "row"), None), P(), P(None, None, "ang"))
    return jax.shard_map(
        body, mesh=mesh, in_specs=placed, out_specs=P(("scan", "row"), "ang"), check_vma=False
    )
```

```python
import functools

import jax
import jax.numpy as jnp
import numpy as np
from jax import lax
from jax.experimental import pallas as pl
from jax.experimental.pallas import tpu as pltpu
from jax.sharding import PartitionSpec as P

HALO = 4
LANES = 128
FLAT_CUTS = 1
TABLE_CUTS = 2
CENTRE = 10
EARLY = 4
paganin_beta = 8.0
ramp_gain = 320.0


def filter_table(tile_rows, width, columns):
    u = np.arange(tile_rows, dtype=np.float64)
    v = np.arange(width, dtype=np.float64)
    lam = (4.0 * np.sin(np.pi * u / tile_rows) ** 2)[:, None] + (4.0 * np.sin(np.pi * v / width) ** 2)[None, :]
    folded = np.minimum(v, width - v)
    ramp = ramp_gain * (folded / width) * (0.5 + 0.5 * np.cos(2.0 * np.pi * folded / width))
    taps = np.real(np.fft.ifft2(ramp[None, :] / (1.0 + paganin_beta * lam)))
    lags = tile_rows // 2 + 1
    place = (np.arange(columns)[:, None] - np.arange(width)[None, :]) % width
    sign = np.where(np.arange(width) < width // LANES // 2 * LANES, 1.0, -1.0)
    return taps[:lags][:, place].reshape(lags * columns, width) * sign


def kernel(regions, tiles, starts, proj, flats, table, weights, out,
           starts_s, proj_v, flats_v, table_v, weights_v, xs, ys, sbuf, rbuf,
           load_sem, done_sem):
    rows, width = flats.shape
    blocks = width // LANES
    angles, cb, _ = weights.shape
    half = rows // 2
    cs = LANES // (2 * rows)
    shifts = cb // cs
    pairs = shifts // 2
    lags = rows + 1
    order = [(0, 0), (1, 0), *[(0, d) for d in range(1, rows)], (1, rows - 1), *[(1, d) for d in range(1, rows - 1)]]
    me = lax.axis_index("ang")
    row = lax.axis_index("row")

    def peer(step, delta):
        return {"ang": lax.rem(me + step, regions), "row": lax.rem(row + delta + tiles, tiles)}

    def when_there(delta, action):
        if delta == 0:
            action()
        else:
            pl.when(row > 0 if delta < 0 else row < tiles - 1)(action)

    start_load = pltpu.make_async_copy(starts, starts_s, load_sem.at[2])
    table_load = pltpu.make_async_copy(table, table_v, load_sem.at[3])
    weight_load = pltpu.make_async_copy(weights, weights_v, done_sem.at[0])

    def load_columns(begin, end, cuts, sem):
        for n in range(cuts):
            part = pl.ds((begin + n * (end - begin) // cuts) * LANES, (end - begin) // cuts * LANES)
            pltpu.make_async_copy(flats.at[:, part], flats_v.at[:, part], sem).start()
        part = pl.ds(begin * LANES, (end - begin) * LANES)
        pltpu.make_async_copy(proj.at[0, :, part], proj_v.at[:, part], sem).start()

    def columns_loaded(count, sem):
        both = xs.at[pl.ds(0, count * 3 // 2)]
        pltpu.make_async_copy(both, both, sem).wait()

    load_columns(0, CENTRE, 1, load_sem.at[0])
    load_columns(CENTRE, blocks, FLAT_CUTS, load_sem.at[1])
    start_load.start()
    for d in range(lags):
        for n in range(TABLE_CUTS):
            part = pl.ds(n * width // TABLE_CUTS, width // TABLE_CUTS)
            pltpu.make_async_copy(table.at[pl.ds(d * cs, cs), part], table_v.at[pl.ds(d * cs, cs), part], load_sem.at[3]).start()
    weight_load.start()

    barrier = pltpu.get_barrier_semaphore()
    def greet(delta):
        for step in range(regions):
            if (step, delta) != (0, 0):
                pl.semaphore_signal(barrier, inc=1, device_id=peer(step, delta), device_id_type=pl.DeviceIdType.MESH)

    for delta in (-1, 0, 1):
        when_there(delta, lambda: greet(delta))

    def slot(delta):
        return pl.ds((1 + delta) * rows, rows)

    zeros = jnp.zeros((angles, rows, pairs * LANES), jnp.bfloat16)
    pl.when(row == tiles - 1)(lambda: rbuf.at[:, slot(-1)].__setitem__(..., zeros))
    pl.when(row == 0)(lambda: rbuf.at[:, slot(1)].__setitem__(..., zeros))

    lane = lax.broadcasted_iota(jnp.int32, (rows, LANES), 1)
    sub = lax.broadcasted_iota(jnp.int32, (rows, LANES), 0)

    pieces = [slice(b * LANES, (b + 1) * LANES) for b in range(blocks)]

    def contrast_of(p):
        return 1.0 - proj_v[:, p].astype(jnp.float32) / flats_v[:, p]

    columns_loaded(CENTRE, load_sem.at[0])
    contrast = [contrast_of(p) for p in pieces[:CENTRE]]
    centre = jnp.sum(sum(contrast), axis=1, keepdims=True) / (CENTRE * LANES)
    columns_loaded(blocks - CENTRE, load_sem.at[1])
    start_load.wait()

    contrast += [contrast_of(p) for p in pieces[CENTRE:]]
    for b, x in enumerate(contrast):
        xs[b] = x - centre
        xs[b + blocks] = x - centre

    spot = lane // cs
    lag = jnp.where(spot < 2, 0, jnp.where(spot < rows, spot - 1, jnp.where(spot < rows + 2, rows - 1, spot - rows - 1)))
    odd = (spot == 1) | (spot > rows)
    up, down = lax.rem(sub + rows - lag, rows), lax.rem(sub + lag, rows)
    inside = [sub >= lag, (lag > 0) & (sub + lag < rows)]
    wrapped = [(sub < lag) | (lag == 0), sub + lag >= rows]
    parts = {-1: [wrapped[0] & (up < half), wrapped[1] & (down < half)],
             1: [wrapped[0] & (up >= half), wrapped[1] & (down >= half)],
             0: inside}
    bits = [1 << n for n in range((rows - 1).bit_length())]
    deep = shifts * rows

    def shifted_rows(group, members=range(blocks)):
        used = sorted({b + n for b in members for n in (0, 1)})
        for region in group:
            shifted = []
            for k in range(shifts):
                start = starts_s[me, region] + k * cs
                first = start // LANES
                rest = lax.rem(start, LANES)
                shift = lax.rem(LANES - rest, LANES)
                low = lane < LANES - rest
                turned = {b: pltpu.roll(xs[first + b], shift, 1) for b in used}
                shifted.append({b: jnp.where(low, turned[b], turned[b + 1]) for b in members})
            for b in members:
                place = region * deep
                ys[place:place + deep, pieces[b]] = jnp.concatenate(
                    [y[b] for y in shifted], axis=0).astype(jnp.bfloat16)

    def filtered(group):
        cut = blocks // 2 * LANES
        begin = group[0] * deep
        end = begin + len(group) * deep
        near, far = (lax.dot_general(
            ys[begin:end, part], jnp.concatenate([table_v[d * cs:(d + 1) * cs, part] for _, d in [*order, (0, rows), (1, rows)]], axis=0),
            (((1,), (1,)), ((), ())), preferred_element_type=jnp.float32) for part in (slice(cut), slice(cut, width)))
        total = near - far
        total = jnp.concatenate([total, jnp.zeros((total.shape[0], LANES - 2 * cs), jnp.float32)], axis=1)
        for n, region in enumerate(group):
            for k in range(pairs):
                base = n * deep + k * 2 * rows
                even_rows, odd_rows = total[base:base + rows], total[base + rows:base + 2 * rows]
                tile = jnp.where(odd, odd_rows[:, :LANES], even_rows[:, :LANES])
                last = jnp.where(odd, odd_rows[:, LANES:], even_rows[:, LANES:])
                ahead, back = tile, tile
                for bit in bits:
                    turn = (lag & bit) > 0
                    ahead = jnp.where(turn, pltpu.roll(ahead, bit, 0), ahead)
                    back = jnp.where(turn, pltpu.roll(back, rows - bit, 0), back)
                edge = jnp.where(lag == 0, last, ahead)
                for delta, (first, second) in parts.items():
                    value = jnp.where(first, edge if delta else ahead, 0.0) + jnp.where(second, back, 0.0)
                    sbuf[(1 + delta) * regions + region, :, k * LANES:(k + 1) * LANES] = value.astype(jnp.bfloat16)

    def send(group):
        for region in group:
            last = (region + (regions - 1 if region < regions // 2 else 1)) % regions
            final = (me == last).astype(jnp.int32)
            for delta in (-1, 1, 0):
                copy = pltpu.make_async_remote_copy(
                    src_ref=sbuf.at[(1 + delta) * regions + region], dst_ref=rbuf.at[me, slot(delta)],
                    send_sem=done_sem.at[0], recv_sem=done_sem.at[final],
                    device_id={"ang": region, "row": lax.rem(row + delta + tiles, tiles)},
                    device_id_type=pl.DeviceIdType.MESH)
                if delta == 0:
                    pl.when(me != region)(copy.start)
                else:
                    when_there(delta, copy.start)

    early = [b for b in range(blocks) if b % (blocks // 2) < EARLY]
    shifted_rows([0], early)
    table_load.wait()
    shifted_rows([0], [b for b in range(blocks) if b not in early])
    filtered([0])
    sides = (row > 0).astype(jnp.int32) + (row < tiles - 1).astype(jnp.int32)
    pl.semaphore_wait(barrier, regions - 1 + sides * regions)
    send([0])
    shifted_rows([*range(1, regions)])
    filtered([*range(1, regions)])
    send([*range(1, regions)])
    rbuf[me, slot(0)] = sbuf[regions + me]

    inner = (row > 0) & (row < tiles - 1)
    turn = jnp.where(me < regions // 2, 1, regions - 1)

    def source(step):
        return lax.rem(me + step * turn, regions)

    def settled(full, short, sem):
        def wait(count):
            units = sbuf.at[pl.ds(0, count)]
            pltpu.make_async_copy(units, units, done_sem.at[sem]).wait()

        pl.when(inner)(lambda: wait(full))
        pl.when(jnp.logical_not(inner))(lambda: wait(short))

    def projected(steps):
        sums = []
        for half_pixels in range(2):
            pixels = pl.ds(half_pixels * (out.shape[1] // 2), out.shape[1] // 2)
            result = 0.0
            for step in steps:
                angle = source(step)
                w = jnp.concatenate(
                    [weights_v[angle, (2 * k + side) * cs:(2 * k + side + 1) * cs, pixels]
                     for k in range(pairs) for side, _ in order], axis=0)
                result += jnp.dot(rbuf[angle], w, preferred_element_type=jnp.float32)
            sums.append(result[:rows] + result[rows:2 * rows] + result[2 * rows:])
        return jnp.concatenate(sums, axis=1)

    loaded = angles * cb * out.shape[1] // (rows * pairs * LANES)
    settled(loaded + 6 * regions - 5, loaded + 4 * regions - 4, 0)
    out[...] = projected(range(regions - 1))
    settled(3, 2, 1)
    out[...] += projected([regions - 1])


def body(projections, flats, block_start, bp_weights):
    _, rows, width = projections.shape
    angles, cb, pixels = bp_weights.shape
    regions, tiles = lax.axis_size("ang"), lax.axis_size("row")
    cs = LANES // (2 * rows)
    pairs = cb // cs // 2
    table = jnp.asarray(filter_table(rows + 2 * HALO, width, cs), jnp.bfloat16)
    hbm = pl.BlockSpec(memory_space=pltpu.HBM)
    return pl.pallas_call(
        functools.partial(kernel, regions, tiles),
        name="fbp",
        out_shape=pltpu.VMEM((rows, pixels), jnp.float32),
        in_specs=[hbm, hbm, hbm, hbm, hbm],
        out_specs=pl.BlockSpec(memory_space=pltpu.VMEM),
        scratch_shapes=[
            pltpu.SMEM(block_start.shape, jnp.int32),
            pltpu.VMEM((rows, width), jnp.bfloat16),
            pltpu.VMEM((rows, width), jnp.float32),
            pltpu.VMEM(table.shape, jnp.bfloat16),
            pltpu.VMEM(bp_weights.shape, jnp.bfloat16),
            pltpu.VMEM((2 * width // LANES, rows, LANES), jnp.float32),
            pltpu.VMEM((regions * (cb // cs) * rows, width), jnp.bfloat16),
            pltpu.VMEM((6 * regions + bp_weights.size // (rows * pairs * LANES), rows, pairs * LANES), jnp.bfloat16),
            pltpu.VMEM((angles, 3 * rows, pairs * LANES), jnp.bfloat16),
            pltpu.SemaphoreType.DMA((4,)),
            pltpu.SemaphoreType.DMA((2,)),
        ],
        compiler_params=pltpu.CompilerParams(collective_id=0, has_side_effects=True, vmem_limit_bytes=65000000),
    )(block_start, projections, flats, table, bp_weights)


def solution(mesh):
    placed = (P(("scan", "ang"), "row", None), P(("scan", "row"), None), P(), P(None, None, "ang"))
    return jax.shard_map(
        body, mesh=mesh, in_specs=placed, out_specs=P(("scan", "row"), "ang"), check_vma=False
    )
```

```python
import functools

import jax
import jax.numpy as jnp
import numpy as np
from jax import lax
from jax.experimental import pallas as pl
from jax.experimental.pallas import tpu as pltpu
from jax.sharding import PartitionSpec as P

HALO = 4
LANES = 128
FLAT_CUTS = 2
TABLE_CUTS = 4
CENTRE = 10
EARLY = 4
paganin_beta = 8.0
ramp_gain = 320.0


def filter_table(tile_rows, width, columns):
    u = np.arange(tile_rows, dtype=np.float64)
    v = np.arange(width, dtype=np.float64)
    lam = (4.0 * np.sin(np.pi * u / tile_rows) ** 2)[:, None] + (4.0 * np.sin(np.pi * v / width) ** 2)[None, :]
    folded = np.minimum(v, width - v)
    ramp = ramp_gain * (folded / width) * (0.5 + 0.5 * np.cos(2.0 * np.pi * folded / width))
    taps = np.real(np.fft.ifft2(ramp[None, :] / (1.0 + paganin_beta * lam)))
    lags = tile_rows // 2 + 1
    place = (np.arange(columns)[:, None] - np.arange(width)[None, :]) % width
    sign = np.where(np.arange(width) < width // LANES // 2 * LANES, 1.0, -1.0)
    return taps[:lags][:, place].reshape(lags * columns, width) * sign


def kernel(regions, tiles, starts, proj, flats, table, weights, out,
           starts_s, proj_v, flats_v, table_v, weights_v, xs, ys, sbuf, rbuf,
           load_sem, done_sem):
    rows, width = flats.shape
    blocks = width // LANES
    angles, cb, _ = weights.shape
    half = rows // 2
    cs = LANES // (2 * rows)
    shifts = cb // cs
    pairs = shifts // 2
    lags = rows + 1
    order = [(0, 0), (1, 0), *[(0, d) for d in range(1, rows)], (1, rows - 1), *[(1, d) for d in range(1, rows - 1)]]
    me = lax.axis_index("ang")
    row = lax.axis_index("row")

    def peer(step, delta):
        return {"ang": lax.rem(me + step, regions), "row": lax.rem(row + delta + tiles, tiles)}

    def when_there(delta, action):
        if delta == 0:
            action()
        else:
            pl.when(row > 0 if delta < 0 else row < tiles - 1)(action)

    start_load = pltpu.make_async_copy(starts, starts_s, load_sem.at[2])
    table_load = pltpu.make_async_copy(table, table_v, load_sem.at[3])
    weight_load = pltpu.make_async_copy(weights, weights_v, done_sem.at[0])

    def load_columns(begin, end, cuts, sem):
        for n in range(cuts):
            part = pl.ds((begin + n * (end - begin) // cuts) * LANES, (end - begin) // cuts * LANES)
            pltpu.make_async_copy(flats.at[:, part], flats_v.at[:, part], sem).start()
        part = pl.ds(begin * LANES, (end - begin) * LANES)
        pltpu.make_async_copy(proj.at[0, :, part], proj_v.at[:, part], sem).start()

    def columns_loaded(count, sem):
        both = xs.at[pl.ds(0, count * 3 // 2)]
        pltpu.make_async_copy(both, both, sem).wait()

    load_columns(0, CENTRE, 1, load_sem.at[0])
    load_columns(CENTRE, blocks, FLAT_CUTS, load_sem.at[1])
    start_load.start()
    for d in range(lags):
        for n in range(TABLE_CUTS):
            part = pl.ds(n * width // TABLE_CUTS, width // TABLE_CUTS)
            pltpu.make_async_copy(table.at[pl.ds(d * cs, cs), part], table_v.at[pl.ds(d * cs, cs), part], load_sem.at[3]).start()
    weight_load.start()

    barrier = pltpu.get_barrier_semaphore()
    def greet(delta):
        for step in range(regions):
            if (step, delta) != (0, 0):
                pl.semaphore_signal(barrier, inc=1, device_id=peer(step, delta), device_id_type=pl.DeviceIdType.MESH)

    for delta in (-1, 0, 1):
        when_there(delta, lambda: greet(delta))

    def slot(delta):
        return pl.ds((1 + delta) * rows, rows)

    zeros = jnp.zeros((angles, rows, pairs * LANES), jnp.bfloat16)
    pl.when(row == tiles - 1)(lambda: rbuf.at[:, slot(-1)].__setitem__(..., zeros))
    pl.when(row == 0)(lambda: rbuf.at[:, slot(1)].__setitem__(..., zeros))

    lane = lax.broadcasted_iota(jnp.int32, (rows, LANES), 1)
    sub = lax.broadcasted_iota(jnp.int32, (rows, LANES), 0)

    pieces = [slice(b * LANES, (b + 1) * LANES) for b in range(blocks)]

    def contrast_of(p):
        return 1.0 - proj_v[:, p].astype(jnp.float32) / flats_v[:, p]

    columns_loaded(CENTRE, load_sem.at[0])
    contrast = [contrast_of(p) for p in pieces[:CENTRE]]
    centre = jnp.sum(sum(contrast), axis=1, keepdims=True) / (CENTRE * LANES)
    columns_loaded(blocks - CENTRE, load_sem.at[1])
    start_load.wait()

    contrast += [contrast_of(p) for p in pieces[CENTRE:]]
    for b, x in enumerate(contrast):
        xs[b] = x - centre
        xs[b + blocks] = x - centre

    spot = lane // cs
    lag = jnp.where(spot < 2, 0, jnp.where(spot < rows, spot - 1, jnp.where(spot < rows + 2, rows - 1, spot - rows - 1)))
    odd = (spot == 1) | (spot > rows)
    up, down = lax.rem(sub + rows - lag, rows), lax.rem(sub + lag, rows)
    inside = [sub >= lag, (lag > 0) & (sub + lag < rows)]
    wrapped = [(sub < lag) | (lag == 0), sub + lag >= rows]
    parts = {-1: [wrapped[0] & (up < half), wrapped[1] & (down < half)],
             1: [wrapped[0] & (up >= half), wrapped[1] & (down >= half)],
             0: inside}
    bits = [1 << n for n in range((rows - 1).bit_length())]
    deep = shifts * rows

    def shifted_rows(group, members=range(blocks)):
        used = sorted({b + n for b in members for n in (0, 1)})
        for region in group:
            shifted = []
            for k in range(shifts):
                start = starts_s[me, region] + k * cs
                first = start // LANES
                rest = lax.rem(start, LANES)
                shift = lax.rem(LANES - rest, LANES)
                low = lane < LANES - rest
                turned = {b: pltpu.roll(xs[first + b], shift, 1) for b in used}
                shifted.append({b: jnp.where(low, turned[b], turned[b + 1]) for b in members})
            for b in members:
                place = region * deep
                ys[place:place + deep, pieces[b]] = jnp.concatenate(
                    [y[b] for y in shifted], axis=0).astype(jnp.bfloat16)

    def filtered(group):
        cut = blocks // 2 * LANES
        begin = group[0] * deep
        end = begin + len(group) * deep
        near, far = (lax.dot_general(
            ys[begin:end, part], jnp.concatenate([table_v[d * cs:(d + 1) * cs, part] for _, d in [*order, (0, rows), (1, rows)]], axis=0),
            (((1,), (1,)), ((), ())), preferred_element_type=jnp.float32) for part in (slice(cut), slice(cut, width)))
        total = near - far
        total = jnp.concatenate([total, jnp.zeros((total.shape[0], LANES - 2 * cs), jnp.float32)], axis=1)
        for n, region in enumerate(group):
            for k in range(pairs):
                base = n * deep + k * 2 * rows
                even_rows, odd_rows = total[base:base + rows], total[base + rows:base + 2 * rows]
                tile = jnp.where(odd, odd_rows[:, :LANES], even_rows[:, :LANES])
                last = jnp.where(odd, odd_rows[:, LANES:], even_rows[:, LANES:])
                ahead, back = tile, tile
                for bit in bits:
                    turn = (lag & bit) > 0
                    ahead = jnp.where(turn, pltpu.roll(ahead, bit, 0), ahead)
                    back = jnp.where(turn, pltpu.roll(back, rows - bit, 0), back)
                edge = jnp.where(lag == 0, last, ahead)
                for delta, (first, second) in parts.items():
                    value = jnp.where(first, edge if delta else ahead, 0.0) + jnp.where(second, back, 0.0)
                    sbuf[(1 + delta) * regions + region, :, k * LANES:(k + 1) * LANES] = value.astype(jnp.bfloat16)

    def send(group):
        for region in group:
            last = (region + (regions - 1 if region < regions // 2 else 1)) % regions
            final = (me == last).astype(jnp.int32)
            for delta in (-1, 1, 0):
                copy = pltpu.make_async_remote_copy(
                    src_ref=sbuf.at[(1 + delta) * regions + region], dst_ref=rbuf.at[me, slot(delta)],
                    send_sem=done_sem.at[0], recv_sem=done_sem.at[final],
                    device_id={"ang": region, "row": lax.rem(row + delta + tiles, tiles)},
                    device_id_type=pl.DeviceIdType.MESH)
                if delta == 0:
                    pl.when(me != region)(copy.start)
                else:
                    when_there(delta, copy.start)

    early = [b for b in range(blocks) if b % (blocks // 2) < EARLY]
    shifted_rows([0], early)
    table_load.wait()
    shifted_rows([0], [b for b in range(blocks) if b not in early])
    filtered([0])
    sides = (row > 0).astype(jnp.int32) + (row < tiles - 1).astype(jnp.int32)
    pl.semaphore_wait(barrier, regions - 1 + sides * regions)
    send([0])
    shifted_rows([*range(1, regions)])
    filtered([*range(1, regions)])
    send([*range(1, regions)])
    rbuf[me, slot(0)] = sbuf[regions + me]

    inner = (row > 0) & (row < tiles - 1)
    turn = jnp.where(me < regions // 2, 1, regions - 1)

    def source(step):
        return lax.rem(me + step * turn, regions)

    def settled(full, short, sem):
        def wait(count):
            units = sbuf.at[pl.ds(0, count)]
            pltpu.make_async_copy(units, units, done_sem.at[sem]).wait()

        pl.when(inner)(lambda: wait(full))
        pl.when(jnp.logical_not(inner))(lambda: wait(short))

    def projected(steps):
        sums = []
        for half_pixels in range(2):
            pixels = pl.ds(half_pixels * (out.shape[1] // 2), out.shape[1] // 2)
            result = 0.0
            for step in steps:
                angle = source(step)
                w = jnp.concatenate(
                    [weights_v[angle, (2 * k + side) * cs:(2 * k + side + 1) * cs, pixels]
                     for k in range(pairs) for side, _ in order], axis=0)
                result += jnp.dot(rbuf[angle], w, preferred_element_type=jnp.float32)
            sums.append(result[:rows] + result[rows:2 * rows] + result[2 * rows:])
        return jnp.concatenate(sums, axis=1)

    loaded = angles * cb * out.shape[1] // (rows * pairs * LANES)
    settled(loaded + 6 * regions - 5, loaded + 4 * regions - 4, 0)
    out[...] = projected(range(regions - 1))
    settled(3, 2, 1)
    out[...] += projected([regions - 1])


def body(projections, flats, block_start, bp_weights):
    _, rows, width = projections.shape
    angles, cb, pixels = bp_weights.shape
    regions, tiles = lax.axis_size("ang"), lax.axis_size("row")
    cs = LANES // (2 * rows)
    pairs = cb // cs // 2
    table = jnp.asarray(filter_table(rows + 2 * HALO, width, cs), jnp.bfloat16)
    hbm = pl.BlockSpec(memory_space=pltpu.HBM)
    return pl.pallas_call(
        functools.partial(kernel, regions, tiles),
        name="fbp",
        out_shape=pltpu.VMEM((rows, pixels), jnp.float32),
        in_specs=[hbm, hbm, hbm, hbm, hbm],
        out_specs=pl.BlockSpec(memory_space=pltpu.VMEM),
        scratch_shapes=[
            pltpu.SMEM(block_start.shape, jnp.int32),
            pltpu.VMEM((rows, width), jnp.bfloat16),
            pltpu.VMEM((rows, width), jnp.float32),
            pltpu.VMEM(table.shape, jnp.bfloat16),
            pltpu.VMEM(bp_weights.shape, jnp.bfloat16),
            pltpu.VMEM((2 * width // LANES, rows, LANES), jnp.float32),
            pltpu.VMEM((regions * (cb // cs) * rows, width), jnp.bfloat16),
            pltpu.VMEM((6 * regions + bp_weights.size // (rows * pairs * LANES), rows, pairs * LANES), jnp.bfloat16),
            pltpu.VMEM((angles, 3 * rows, pairs * LANES), jnp.bfloat16),
            pltpu.SemaphoreType.DMA((4,)),
            pltpu.SemaphoreType.DMA((2,)),
        ],
        compiler_params=pltpu.CompilerParams(collective_id=0, has_side_effects=True, vmem_limit_bytes=65000000),
    )(block_start, projections, flats, table, bp_weights)


def solution(mesh):
    placed = (P(("scan", "ang"), "row", None), P(("scan", "row"), None), P(), P(None, None, "ang"))
    return jax.shard_map(
        body, mesh=mesh, in_specs=placed, out_specs=P(("scan", "row"), "ang"), check_vma=False
    )
```

```python
import functools

import jax
import jax.numpy as jnp
import numpy as np
from jax import lax
from jax.experimental import pallas as pl
from jax.experimental.pallas import tpu as pltpu
from jax.sharding import PartitionSpec as P

HALO = 4
LANES = 128
FLAT_CUTS = 2
TABLE_CUTS = 2
CENTRE = 8
EARLY = 6
paganin_beta = 8.0
ramp_gain = 320.0


def filter_table(tile_rows, width, columns):
    u = np.arange(tile_rows, dtype=np.float64)
    v = np.arange(width, dtype=np.float64)
    lam = (4.0 * np.sin(np.pi * u / tile_rows) ** 2)[:, None] + (4.0 * np.sin(np.pi * v / width) ** 2)[None, :]
    folded = np.minimum(v, width - v)
    ramp = ramp_gain * (folded / width) * (0.5 + 0.5 * np.cos(2.0 * np.pi * folded / width))
    taps = np.real(np.fft.ifft2(ramp[None, :] / (1.0 + paganin_beta * lam)))
    lags = tile_rows // 2 + 1
    place = (np.arange(columns)[:, None] - np.arange(width)[None, :]) % width
    sign = np.where(np.arange(width) < width // LANES // 2 * LANES, 1.0, -1.0)
    return taps[:lags][:, place].reshape(lags * columns, width) * sign


def kernel(regions, tiles, starts, proj, flats, table, weights, out,
           starts_s, proj_v, flats_v, table_v, weights_v, xs, ys, sbuf, rbuf,
           load_sem, done_sem):
    rows, width = flats.shape
    blocks = width // LANES
    angles, cb, _ = weights.shape
    half = rows // 2
    cs = LANES // (2 * rows)
    shifts = cb // cs
    pairs = shifts // 2
    lags = rows + 1
    order = [(0, 0), (1, 0), *[(0, d) for d in range(1, rows)], (1, rows - 1), *[(1, d) for d in range(1, rows - 1)]]
    me = lax.axis_index("ang")
    row = lax.axis_index("row")

    def peer(step, delta):
        return {"ang": lax.rem(me + step, regions), "row": lax.rem(row + delta + tiles, tiles)}

    def when_there(delta, action):
        if delta == 0:
            action()
        else:
            pl.when(row > 0 if delta < 0 else row < tiles - 1)(action)

    start_load = pltpu.make_async_copy(starts, starts_s, load_sem.at[2])
    table_load = pltpu.make_async_copy(table, table_v, load_sem.at[3])
    weight_load = pltpu.make_async_copy(weights, weights_v, done_sem.at[0])

    def load_columns(begin, end, cuts, sem):
        for n in range(cuts):
            part = pl.ds((begin + n * (end - begin) // cuts) * LANES, (end - begin) // cuts * LANES)
            pltpu.make_async_copy(flats.at[:, part], flats_v.at[:, part], sem).start()
        part = pl.ds(begin * LANES, (end - begin) * LANES)
        pltpu.make_async_copy(proj.at[0, :, part], proj_v.at[:, part], sem).start()

    def columns_loaded(count, sem):
        both = xs.at[pl.ds(0, count * 3 // 2)]
        pltpu.make_async_copy(both, both, sem).wait()

    load_columns(0, CENTRE, 1, load_sem.at[0])
    load_columns(CENTRE, blocks, FLAT_CUTS, load_sem.at[1])
    start_load.start()
    for d in range(lags):
        for n in range(TABLE_CUTS):
            part = pl.ds(n * width // TABLE_CUTS, width // TABLE_CUTS)
            pltpu.make_async_copy(table.at[pl.ds(d * cs, cs), part], table_v.at[pl.ds(d * cs, cs), part], load_sem.at[3]).start()
    weight_load.start()

    barrier = pltpu.get_barrier_semaphore()
    def greet(delta):
        for step in range(regions):
            if (step, delta) != (0, 0):
                pl.semaphore_signal(barrier, inc=1, device_id=peer(step, delta), device_id_type=pl.DeviceIdType.MESH)

    for delta in (-1, 0, 1):
        when_there(delta, lambda: greet(delta))

    def slot(delta):
        return pl.ds((1 + delta) * rows, rows)

    zeros = jnp.zeros((angles, rows, pairs * LANES), jnp.bfloat16)
    pl.when(row == tiles - 1)(lambda: rbuf.at[:, slot(-1)].__setitem__(..., zeros))
    pl.when(row == 0)(lambda: rbuf.at[:, slot(1)].__setitem__(..., zeros))

    lane = lax.broadcasted_iota(jnp.int32, (rows, LANES), 1)
    sub = lax.broadcasted_iota(jnp.int32, (rows, LANES), 0)

    pieces = [slice(b * LANES, (b + 1) * LANES) for b in range(blocks)]

    def contrast_of(p):
        return 1.0 - proj_v[:, p].astype(jnp.float32) / flats_v[:, p]

    columns_loaded(CENTRE, load_sem.at[0])
    contrast = [contrast_of(p) for p in pieces[:CENTRE]]
    centre = jnp.sum(sum(contrast), axis=1, keepdims=True) / (CENTRE * LANES)
    columns_loaded(blocks - CENTRE, load_sem.at[1])
    start_load.wait()

    contrast += [contrast_of(p) for p in pieces[CENTRE:]]
    for b, x in enumerate(contrast):
        xs[b] = x - centre
        xs[b + blocks] = x - centre

    spot = lane // cs
    lag = jnp.where(spot < 2, 0, jnp.where(spot < rows, spot - 1, jnp.where(spot < rows + 2, rows - 1, spot - rows - 1)))
    odd = (spot == 1) | (spot > rows)
    up, down = lax.rem(sub + rows - lag, rows), lax.rem(sub + lag, rows)
    inside = [sub >= lag, (lag > 0) & (sub + lag < rows)]
    wrapped = [(sub < lag) | (lag == 0), sub + lag >= rows]
    parts = {-1: [wrapped[0] & (up < half), wrapped[1] & (down < half)],
             1: [wrapped[0] & (up >= half), wrapped[1] & (down >= half)],
             0: inside}
    bits = [1 << n for n in range((rows - 1).bit_length())]
    deep = shifts * rows

    def shifted_rows(group, members=range(blocks)):
        used = sorted({b + n for b in members for n in (0, 1)})
        for region in group:
            shifted = []
            for k in range(shifts):
                start = starts_s[me, region] + k * cs
                first = start // LANES
                rest = lax.rem(start, LANES)
                shift = lax.rem(LANES - rest, LANES)
                low = lane < LANES - rest
                turned = {b: pltpu.roll(xs[first + b], shift, 1) for b in used}
                shifted.append({b: jnp.where(low, turned[b], turned[b + 1]) for b in members})
            for b in members:
                place = region * deep
                ys[place:place + deep, pieces[b]] = jnp.concatenate(
                    [y[b] for y in shifted], axis=0).astype(jnp.bfloat16)

    def filtered(group):
        cut = blocks // 2 * LANES
        begin = group[0] * deep
        end = begin + len(group) * deep
        near, far = (lax.dot_general(
            ys[begin:end, part], jnp.concatenate([table_v[d * cs:(d + 1) * cs, part] for _, d in [*order, (0, rows), (1, rows)]], axis=0),
            (((1,), (1,)), ((), ())), preferred_element_type=jnp.float32) for part in (slice(cut), slice(cut, width)))
        total = near - far
        total = jnp.concatenate([total, jnp.zeros((total.shape[0], LANES - 2 * cs), jnp.float32)], axis=1)
        for n, region in enumerate(group):
            for k in range(pairs):
                base = n * deep + k * 2 * rows
                even_rows, odd_rows = total[base:base + rows], total[base + rows:base + 2 * rows]
                tile = jnp.where(odd, odd_rows[:, :LANES], even_rows[:, :LANES])
                last = jnp.where(odd, odd_rows[:, LANES:], even_rows[:, LANES:])
                ahead, back = tile, tile
                for bit in bits:
                    turn = (lag & bit) > 0
                    ahead = jnp.where(turn, pltpu.roll(ahead, bit, 0), ahead)
                    back = jnp.where(turn, pltpu.roll(back, rows - bit, 0), back)
                edge = jnp.where(lag == 0, last, ahead)
                for delta, (first, second) in parts.items():
                    value = jnp.where(first, edge if delta else ahead, 0.0) + jnp.where(second, back, 0.0)
                    sbuf[(1 + delta) * regions + region, :, k * LANES:(k + 1) * LANES] = value.astype(jnp.bfloat16)

    def send(group):
        for region in group:
            last = (region + (regions - 1 if region < regions // 2 else 1)) % regions
            final = (me == last).astype(jnp.int32)
            for delta in (-1, 1, 0):
                copy = pltpu.make_async_remote_copy(
                    src_ref=sbuf.at[(1 + delta) * regions + region], dst_ref=rbuf.at[me, slot(delta)],
                    send_sem=done_sem.at[0], recv_sem=done_sem.at[final],
                    device_id={"ang": region, "row": lax.rem(row + delta + tiles, tiles)},
                    device_id_type=pl.DeviceIdType.MESH)
                if delta == 0:
                    pl.when(me != region)(copy.start)
                else:
                    when_there(delta, copy.start)

    early = [b for b in range(blocks) if b % (blocks // 2) < EARLY]
    shifted_rows([0], early)
    table_load.wait()
    shifted_rows([0], [b for b in range(blocks) if b not in early])
    filtered([0])
    sides = (row > 0).astype(jnp.int32) + (row < tiles - 1).astype(jnp.int32)
    pl.semaphore_wait(barrier, regions - 1 + sides * regions)
    send([0])
    shifted_rows([*range(1, regions)])
    filtered([*range(1, regions)])
    send([*range(1, regions)])
    rbuf[me, slot(0)] = sbuf[regions + me]

    inner = (row > 0) & (row < tiles - 1)
    turn = jnp.where(me < regions // 2, 1, regions - 1)

    def source(step):
        return lax.rem(me + step * turn, regions)

    def settled(full, short, sem):
        def wait(count):
            units = sbuf.at[pl.ds(0, count)]
            pltpu.make_async_copy(units, units, done_sem.at[sem]).wait()

        pl.when(inner)(lambda: wait(full))
        pl.when(jnp.logical_not(inner))(lambda: wait(short))

    def projected(steps):
        sums = []
        for half_pixels in range(2):
            pixels = pl.ds(half_pixels * (out.shape[1] // 2), out.shape[1] // 2)
            result = 0.0
            for step in steps:
                angle = source(step)
                w = jnp.concatenate(
                    [weights_v[angle, (2 * k + side) * cs:(2 * k + side + 1) * cs, pixels]
                     for k in range(pairs) for side, _ in order], axis=0)
                result += jnp.dot(rbuf[angle], w, preferred_element_type=jnp.float32)
            sums.append(result[:rows] + result[rows:2 * rows] + result[2 * rows:])
        return jnp.concatenate(sums, axis=1)

    loaded = angles * cb * out.shape[1] // (rows * pairs * LANES)
    settled(loaded + 6 * regions - 5, loaded + 4 * regions - 4, 0)
    out[...] = projected(range(regions - 1))
    settled(3, 2, 1)
    out[...] += projected([regions - 1])


def body(projections, flats, block_start, bp_weights):
    _, rows, width = projections.shape
    angles, cb, pixels = bp_weights.shape
    regions, tiles = lax.axis_size("ang"), lax.axis_size("row")
    cs = LANES // (2 * rows)
    pairs = cb // cs // 2
    table = jnp.asarray(filter_table(rows + 2 * HALO, width, cs), jnp.bfloat16)
    hbm = pl.BlockSpec(memory_space=pltpu.HBM)
    return pl.pallas_call(
        functools.partial(kernel, regions, tiles),
        name="fbp",
        out_shape=pltpu.VMEM((rows, pixels), jnp.float32),
        in_specs=[hbm, hbm, hbm, hbm, hbm],
        out_specs=pl.BlockSpec(memory_space=pltpu.VMEM),
        scratch_shapes=[
            pltpu.SMEM(block_start.shape, jnp.int32),
            pltpu.VMEM((rows, width), jnp.bfloat16),
            pltpu.VMEM((rows, width), jnp.float32),
            pltpu.VMEM(table.shape, jnp.bfloat16),
            pltpu.VMEM(bp_weights.shape, jnp.bfloat16),
            pltpu.VMEM((2 * width // LANES, rows, LANES), jnp.float32),
            pltpu.VMEM((regions * (cb // cs) * rows, width), jnp.bfloat16),
            pltpu.VMEM((6 * regions + bp_weights.size // (rows * pairs * LANES), rows, pairs * LANES), jnp.bfloat16),
            pltpu.VMEM((angles, 3 * rows, pairs * LANES), jnp.bfloat16),
            pltpu.SemaphoreType.DMA((4,)),
            pltpu.SemaphoreType.DMA((2,)),
        ],
        compiler_params=pltpu.CompilerParams(collective_id=0, has_side_effects=True, vmem_limit_bytes=65000000),
    )(block_start, projections, flats, table, bp_weights)


def solution(mesh):
    placed = (P(("scan", "ang"), "row", None), P(("scan", "row"), None), P(), P(None, None, "ang"))
    return jax.shard_map(
        body, mesh=mesh, in_specs=placed, out_specs=P(("scan", "row"), "ang"), check_vma=False
    )
```

```python
import functools

import jax
import jax.numpy as jnp
import numpy as np
from jax import lax
from jax.experimental import pallas as pl
from jax.experimental.pallas import tpu as pltpu
from jax.sharding import PartitionSpec as P

HALO = 4
LANES = 128
FLAT_CUTS = 2
TABLE_CUTS = 2
CENTRE = 8
EARLY = 4
paganin_beta = 8.0
ramp_gain = 320.0


def filter_table(tile_rows, width, columns):
    u = np.arange(tile_rows, dtype=np.float64)
    v = np.arange(width, dtype=np.float64)
    lam = (4.0 * np.sin(np.pi * u / tile_rows) ** 2)[:, None] + (4.0 * np.sin(np.pi * v / width) ** 2)[None, :]
    folded = np.minimum(v, width - v)
    ramp = ramp_gain * (folded / width) * (0.5 + 0.5 * np.cos(2.0 * np.pi * folded / width))
    taps = np.real(np.fft.ifft2(ramp[None, :] / (1.0 + paganin_beta * lam)))
    lags = tile_rows // 2 + 1
    place = (np.arange(columns)[:, None] - np.arange(width)[None, :]) % width
    sign = np.where(np.arange(width) < width // LANES // 2 * LANES, 1.0, -1.0)
    return taps[:lags][:, place].reshape(lags * columns, width) * sign


def kernel(regions, tiles, starts, proj, flats, table, weights, out,
           starts_s, proj_v, flats_v, table_v, weights_v, xs, ys, sbuf, rbuf,
           load_sem, done_sem):
    rows, width = flats.shape
    blocks = width // LANES
    angles, cb, _ = weights.shape
    half = rows // 2
    cs = LANES // (2 * rows)
    shifts = cb // cs
    pairs = shifts // 2
    lags = rows + 1
    order = [(0, 0), (1, 0), *[(0, d) for d in range(1, rows)], (1, rows - 1), *[(1, d) for d in range(1, rows - 1)]]
    me = lax.axis_index("ang")
    row = lax.axis_index("row")

    def peer(step, delta):
        return {"ang": lax.rem(me + step, regions), "row": lax.rem(row + delta + tiles, tiles)}

    def when_there(delta, action):
        if delta == 0:
            action()
        else:
            pl.when(row > 0 if delta < 0 else row < tiles - 1)(action)

    start_load = pltpu.make_async_copy(starts, starts_s, load_sem.at[2])
    table_load = pltpu.make_async_copy(table, table_v, load_sem.at[3])
    weight_load = pltpu.make_async_copy(weights, weights_v, done_sem.at[0])

    def load_columns(begin, end, cuts, sem):
        for n in range(cuts):
            part = pl.ds((begin + n * (end - begin) // cuts) * LANES, (end - begin) // cuts * LANES)
            pltpu.make_async_copy(flats.at[:, part], flats_v.at[:, part], sem).start()
        part = pl.ds(begin * LANES, (end - begin) * LANES)
        pltpu.make_async_copy(proj.at[0, :, part], proj_v.at[:, part], sem).start()

    def columns_loaded(count, sem):
        both = xs.at[pl.ds(0, count * 3 // 2)]
        pltpu.make_async_copy(both, both, sem).wait()

    load_columns(0, CENTRE, 1, load_sem.at[0])
    load_columns(CENTRE, blocks, FLAT_CUTS, load_sem.at[1])
    start_load.start()
    for d in range(lags):
        for n in range(TABLE_CUTS):
            part = pl.ds(n * width // TABLE_CUTS, width // TABLE_CUTS)
            pltpu.make_async_copy(table.at[pl.ds(d * cs, cs), part], table_v.at[pl.ds(d * cs, cs), part], load_sem.at[3]).start()
    weight_load.start()

    barrier = pltpu.get_barrier_semaphore()
    def greet(delta):
        for step in range(regions):
            if (step, delta) != (0, 0):
                pl.semaphore_signal(barrier, inc=1, device_id=peer(step, delta), device_id_type=pl.DeviceIdType.MESH)

    for delta in (-1, 0, 1):
        when_there(delta, lambda: greet(delta))

    def slot(delta):
        return pl.ds((1 + delta) * rows, rows)

    zeros = jnp.zeros((angles, rows, pairs * LANES), jnp.bfloat16)
    pl.when(row == tiles - 1)(lambda: rbuf.at[:, slot(-1)].__setitem__(..., zeros))
    pl.when(row == 0)(lambda: rbuf.at[:, slot(1)].__setitem__(..., zeros))

    lane = lax.broadcasted_iota(jnp.int32, (rows, LANES), 1)
    sub = lax.broadcasted_iota(jnp.int32, (rows, LANES), 0)

    pieces = [slice(b * LANES, (b + 1) * LANES) for b in range(blocks)]

    def contrast_of(p):
        return 1.0 - proj_v[:, p].astype(jnp.float32) / flats_v[:, p]

    columns_loaded(CENTRE, load_sem.at[0])
    contrast = [contrast_of(p) for p in pieces[:CENTRE]]
    centre = jnp.sum(sum(contrast), axis=1, keepdims=True) / (CENTRE * LANES)
    columns_loaded(blocks - CENTRE, load_sem.at[1])
    start_load.wait()

    contrast += [contrast_of(p) for p in pieces[CENTRE:]]
    for b, x in enumerate(contrast):
        xs[b] = x - centre
        xs[b + blocks] = x - centre

    spot = lane // cs
    lag = jnp.where(spot < 2, 0, jnp.where(spot < rows, spot - 1, jnp.where(spot < rows + 2, rows - 1, spot - rows - 1)))
    odd = (spot == 1) | (spot > rows)
    up, down = lax.rem(sub + rows - lag, rows), lax.rem(sub + lag, rows)
    inside = [sub >= lag, (lag > 0) & (sub + lag < rows)]
    wrapped = [(sub < lag) | (lag == 0), sub + lag >= rows]
    parts = {-1: [wrapped[0] & (up < half), wrapped[1] & (down < half)],
             1: [wrapped[0] & (up >= half), wrapped[1] & (down >= half)],
             0: inside}
    bits = [1 << n for n in range((rows - 1).bit_length())]
    deep = shifts * rows

    def shifted_rows(group, members=range(blocks)):
        used = sorted({b + n for b in members for n in (0, 1)})
        for region in group:
            shifted = []
            for k in range(shifts):
                start = starts_s[me, region] + k * cs
                first = start // LANES
                rest = lax.rem(start, LANES)
                shift = lax.rem(LANES - rest, LANES)
                low = lane < LANES - rest
                turned = {b: pltpu.roll(xs[first + b], shift, 1) for b in used}
                shifted.append({b: jnp.where(low, turned[b], turned[b + 1]) for b in members})
            for b in members:
                place = region * deep
                ys[place:place + deep, pieces[b]] = jnp.concatenate(
                    [y[b] for y in shifted], axis=0).astype(jnp.bfloat16)

    def filtered(group):
        cut = blocks // 2 * LANES
        begin = group[0] * deep
        end = begin + len(group) * deep
        near, far = (lax.dot_general(
            ys[begin:end, part], jnp.concatenate([table_v[d * cs:(d + 1) * cs, part] for _, d in [*order, (0, rows), (1, rows)]], axis=0),
            (((1,), (1,)), ((), ())), preferred_element_type=jnp.float32) for part in (slice(cut), slice(cut, width)))
        total = near - far
        total = jnp.concatenate([total, jnp.zeros((total.shape[0], LANES - 2 * cs), jnp.float32)], axis=1)
        for n, region in enumerate(group):
            for k in range(pairs):
                base = n * deep + k * 2 * rows
                even_rows, odd_rows = total[base:base + rows], total[base + rows:base + 2 * rows]
                tile = jnp.where(odd, odd_rows[:, :LANES], even_rows[:, :LANES])
                last = jnp.where(odd, odd_rows[:, LANES:], even_rows[:, LANES:])
                ahead, back = tile, tile
                for bit in bits:
                    turn = (lag & bit) > 0
                    ahead = jnp.where(turn, pltpu.roll(ahead, bit, 0), ahead)
                    back = jnp.where(turn, pltpu.roll(back, rows - bit, 0), back)
                edge = jnp.where(lag == 0, last, ahead)
                for delta, (first, second) in parts.items():
                    value = jnp.where(first, edge if delta else ahead, 0.0) + jnp.where(second, back, 0.0)
                    sbuf[(1 + delta) * regions + region, :, k * LANES:(k + 1) * LANES] = value.astype(jnp.bfloat16)

    def send(group):
        for region in group:
            last = (region + (regions - 1 if region < regions // 2 else 1)) % regions
            final = (me == last).astype(jnp.int32)
            for delta in (-1, 1, 0):
                copy = pltpu.make_async_remote_copy(
                    src_ref=sbuf.at[(1 + delta) * regions + region], dst_ref=rbuf.at[me, slot(delta)],
                    send_sem=done_sem.at[0], recv_sem=done_sem.at[final],
                    device_id={"ang": region, "row": lax.rem(row + delta + tiles, tiles)},
                    device_id_type=pl.DeviceIdType.MESH)
                if delta == 0:
                    pl.when(me != region)(copy.start)
                else:
                    when_there(delta, copy.start)

    early = [b for b in range(blocks) if b % (blocks // 2) < EARLY]
    shifted_rows([0], early)
    table_load.wait()
    shifted_rows([0], [b for b in range(blocks) if b not in early])
    filtered([0])
    sides = (row > 0).astype(jnp.int32) + (row < tiles - 1).astype(jnp.int32)
    pl.semaphore_wait(barrier, regions - 1 + sides * regions)
    send([0])
    shifted_rows([*range(1, regions)])
    filtered([*range(1, regions)])
    send([*range(1, regions)])
    rbuf[me, slot(0)] = sbuf[regions + me]

    inner = (row > 0) & (row < tiles - 1)
    turn = jnp.where(me < regions // 2, 1, regions - 1)

    def source(step):
        return lax.rem(me + step * turn, regions)

    def settled(full, short, sem):
        def wait(count):
            units = sbuf.at[pl.ds(0, count)]
            pltpu.make_async_copy(units, units, done_sem.at[sem]).wait()

        pl.when(inner)(lambda: wait(full))
        pl.when(jnp.logical_not(inner))(lambda: wait(short))

    def projected(steps):
        sums = []
        for half_pixels in range(2):
            pixels = pl.ds(half_pixels * (out.shape[1] // 2), out.shape[1] // 2)
            result = 0.0
            for step in steps:
                angle = source(step)
                w = jnp.concatenate(
                    [weights_v[angle, (2 * k + side) * cs:(2 * k + side + 1) * cs, pixels]
                     for k in range(pairs) for side, _ in order], axis=0)
                result += jnp.dot(rbuf[angle], w, preferred_element_type=jnp.float32)
            sums.append(result[:rows] + result[rows:2 * rows] + result[2 * rows:])
        return jnp.concatenate(sums, axis=1)

    loaded = angles * cb * out.shape[1] // (rows * pairs * LANES)
    settled(loaded + 6 * regions - 5, loaded + 4 * regions - 4, 0)
    out[...] = projected(range(regions - 1))
    settled(3, 2, 1)
    out[...] += projected([regions - 1])


def body(projections, flats, block_start, bp_weights):
    _, rows, width = projections.shape
    angles, cb, pixels = bp_weights.shape
    regions, tiles = lax.axis_size("ang"), lax.axis_size("row")
    cs = LANES // (2 * rows)
    pairs = cb // cs // 2
    table = jnp.asarray(filter_table(rows + 2 * HALO, width, cs), jnp.bfloat16)
    hbm = pl.BlockSpec(memory_space=pltpu.HBM)
    return pl.pallas_call(
        functools.partial(kernel, regions, tiles),
        name="fbp",
        out_shape=pltpu.VMEM((rows, pixels), jnp.float32),
        in_specs=[hbm, hbm, hbm, hbm, hbm],
        out_specs=pl.BlockSpec(memory_space=pltpu.VMEM),
        scratch_shapes=[
            pltpu.SMEM(block_start.shape, jnp.int32),
            pltpu.VMEM((rows, width), jnp.bfloat16),
            pltpu.VMEM((rows, width), jnp.float32),
            pltpu.VMEM(table.shape, jnp.bfloat16),
            pltpu.VMEM(bp_weights.shape, jnp.bfloat16),
            pltpu.VMEM((2 * width // LANES, rows, LANES), jnp.float32),
            pltpu.VMEM((regions * (cb // cs) * rows, width), jnp.bfloat16),
            pltpu.VMEM((6 * regions + bp_weights.size // (rows * pairs * LANES), rows, pairs * LANES), jnp.bfloat16),
            pltpu.VMEM((angles, 3 * rows, pairs * LANES), jnp.bfloat16),
            pltpu.SemaphoreType.DMA((4,)),
            pltpu.SemaphoreType.DMA((2,)),
        ],
        compiler_params=pltpu.CompilerParams(collective_id=0, has_side_effects=True, vmem_limit_bytes=65000000),
    )(block_start, projections, flats, table, bp_weights)


def solution(mesh):
    placed = (P(("scan", "ang"), "row", None), P(("scan", "row"), None), P(), P(None, None, "ang"))
    return jax.shard_map(
        body, mesh=mesh, in_specs=placed, out_specs=P(("scan", "row"), "ang"), check_vma=False
    )
```
